16 devices in a mesh: dp: 2 (over y, z), cp: 8 (over x, core).
Axes of the slice: x: 4, y: 2, z: 1, core: 2. Of those that a mesh axis runs over, the one named last changes fastest.
The devices are a block of a 4x4x8 slice.
Arguments:
- images: bfloat16 [32, 1024, 768], P('dp', 'cp'), parts along dimension 0
- ln1_scale: float32 [768], replicated
- ln1_bias: float32 [768], replicated
- w_qkv: bfloat16 [768, 3, 12, 64], replicated
- b_qkv: float32 [3, 12, 64], replicated
- w_out: bfloat16 [12, 64, 768], replicated
- b_out: float32 [768], replicated
- ln2_scale: float32 [768], replicated
- ln2_bias: float32 [768], replicated
- w_up: bfloat16 [768, 3072], replicated
- b_up: float32 [3072], replicated
- w_down: bfloat16 [3072, 768], replicated
- b_down: float32 [768], replicated
- lnf_scale: float32 [768], replicated
- lnf_bias: float32 [768], replicated
- pool_probe: bfloat16 [1, 768], replicated
- pool_wq: bfloat16 [768, 12, 64], replicated
- pool_bq: float32 [12, 64], replicated
- pool_wkv: bfloat16 [768, 2, 12, 64], replicated
- pool_bkv: float32 [2, 12, 64], replicated
- pool_wout: bfloat16 [12, 64, 768], replicated
- pool_bout: float32 [768], replicated
- pool_ln_scale: float32 [768], replicated
- pool_ln_bias: float32 [768], replicated
- pool_w_up: bfloat16 [768, 3072], replicated
- pool_b_up: float32 [3072], replicated
- pool_w_down: bfloat16 [3072, 768], replicated
- pool_b_down: float32 [768], replicated
Outputs:
- output: float32 [32, 768], P('dp'), parts along dimension 0
There are 2 independent parts. The reference program is written for one: setup_inputs(seed, part) draws one part's arguments, and reference() takes and returns one part's arrays. A program takes and returns all parts, laid end to end along the dimension named above; an argument that names none is the same for every part.
All inputs are finite; a program needn't handle non-finite values.
Results may differ from the reference program's by a relative error of at most 0.0093231.
Values are sent between devices in bfloat16 or wider.
A program may use at most 768 MiB of HBM per device.

```python
import math
import jax
import jax.numpy as jnp
from jax import lax

IMAGES = 16
TOKENS = 1024
MODEL_DIM = 768
NUM_HEADS = 12
HEAD_DIM = 64
MLP_DIM = 3072

ROW_BLOCK = TOKENS // 16
GRID_SIDE = math.isqrt(TOKENS)


def weight_draw(rand_key, arr_shape, fan_in):
    return (jax.random.normal(rand_key, arr_shape, jnp.float32) * fan_in ** -0.5).astype(jnp.bfloat16)


def gain_draw(rand_key, arr_shape):
    return 1.0 + 0.2 * jax.random.normal(rand_key, arr_shape, jnp.float32)


def shift_draw(rand_key, arr_shape):
    return 0.2 * jax.random.normal(rand_key, arr_shape, jnp.float32)


def setup_inputs(seed: int = 0, part: int = 0) -> dict:
    root_key = jax.random.key(seed)
    halves = jax.random.split(root_key, 2)
    image_keys = jax.random.split(jax.random.fold_in(halves[0], part), 5)
    weight_keys = jax.random.split(halves[1], 27)
    wave_count = 8
    positions = jnp.arange(TOKENS)
    grid_rows = (positions // GRID_SIDE).astype(jnp.float32) / GRID_SIDE
    grid_cols = (positions % GRID_SIDE).astype(jnp.float32) / GRID_SIDE
    freq_rows = jax.random.randint(image_keys[0], (IMAGES, wave_count), 1, 4).astype(jnp.float32)
    freq_cols = jax.random.randint(image_keys[1], (IMAGES, wave_count), 0, 4).astype(jnp.float32)
    phases = jax.random.uniform(image_keys[2], (IMAGES, wave_count), jnp.float32, 0.0, 2.0 * math.pi)
    wave_rows = jnp.cos(2.0 * math.pi * (freq_rows[:, :, None] * grid_rows + freq_cols[:, :, None] * grid_cols) + phases[:, :, None])
    directions = jax.random.normal(image_keys[3], (IMAGES, wave_count, MODEL_DIM), jnp.float32) * (2.0 / wave_count) ** 0.5
    wave_field = jnp.einsum("bwn,bwd->bnd", wave_rows, directions)
    noise_part = jax.random.normal(image_keys[4], (IMAGES, TOKENS, MODEL_DIM), jnp.float32)
    return {
        "images": (wave_field + 0.5 * noise_part).astype(jnp.bfloat16),
        "ln1_scale": gain_draw(weight_keys[0], (MODEL_DIM,)),
        "ln1_bias": shift_draw(weight_keys[1], (MODEL_DIM,)),
        "w_qkv": weight_draw(weight_keys[2], (MODEL_DIM, 3, NUM_HEADS, HEAD_DIM), MODEL_DIM),
        "b_qkv": shift_draw(weight_keys[3], (3, NUM_HEADS, HEAD_DIM)),
        "w_out": weight_draw(weight_keys[4], (NUM_HEADS, HEAD_DIM, MODEL_DIM), MODEL_DIM),
        "b_out": shift_draw(weight_keys[5], (MODEL_DIM,)),
        "ln2_scale": gain_draw(weight_keys[6], (MODEL_DIM,)),
        "ln2_bias": shift_draw(weight_keys[7], (MODEL_DIM,)),
        "w_up": weight_draw(weight_keys[8], (MODEL_DIM, MLP_DIM), MODEL_DIM),
        "b_up": shift_draw(weight_keys[9], (MLP_DIM,)),
        "w_down": weight_draw(weight_keys[10], (MLP_DIM, MODEL_DIM), MLP_DIM),
        "b_down": shift_draw(weight_keys[11], (MODEL_DIM,)),
        "lnf_scale": gain_draw(weight_keys[12], (MODEL_DIM,)),
        "lnf_bias": shift_draw(weight_keys[13], (MODEL_DIM,)),
        "pool_probe": jax.random.normal(weight_keys[14], (1, MODEL_DIM), jnp.float32).astype(jnp.bfloat16),
        "pool_wq": weight_draw(weight_keys[15], (MODEL_DIM, NUM_HEADS, HEAD_DIM), MODEL_DIM),
        "pool_bq": shift_draw(weight_keys[16], (NUM_HEADS, HEAD_DIM)),
        "pool_wkv": weight_draw(weight_keys[17], (MODEL_DIM, 2, NUM_HEADS, HEAD_DIM), MODEL_DIM),
        "pool_bkv": shift_draw(weight_keys[18], (2, NUM_HEADS, HEAD_DIM)),
        "pool_wout": weight_draw(weight_keys[19], (NUM_HEADS, HEAD_DIM, MODEL_DIM), MODEL_DIM),
        "pool_bout": shift_draw(weight_keys[20], (MODEL_DIM,)),
        "pool_ln_scale": gain_draw(weight_keys[21], (MODEL_DIM,)),
        "pool_ln_bias": shift_draw(weight_keys[22], (MODEL_DIM,)),
        "pool_w_up": weight_draw(weight_keys[23], (MODEL_DIM, MLP_DIM), MODEL_DIM),
        "pool_b_up": shift_draw(weight_keys[24], (MLP_DIM,)),
        "pool_w_down": weight_draw(weight_keys[25], (MLP_DIM, MODEL_DIM), MLP_DIM),
        "pool_b_down": shift_draw(weight_keys[26], (MODEL_DIM,)),
    }


def layer_norm(values, ln_gain, ln_shift):
    row_mean = jnp.mean(values, axis=-1, keepdims=True)
    centered = values - row_mean
    variance = jnp.mean(centered * centered, axis=-1, keepdims=True)
    return centered * lax.rsqrt(variance + 1e-6) * ln_gain + ln_shift


def reference(images, ln1_scale, ln1_bias, w_qkv, b_qkv, w_out, b_out, ln2_scale, ln2_bias, w_up, b_up, w_down, b_down, lnf_scale, lnf_bias, pool_probe, pool_wq, pool_bq, pool_wkv, pool_bkv, pool_wout, pool_bout, pool_ln_scale, pool_ln_bias, pool_w_up, pool_b_up, pool_w_down, pool_b_down):
    score_scale = HEAD_DIM ** -0.5
    probe_q = (jnp.einsum("od,dhe->he", pool_probe.astype(jnp.float32), pool_wq.astype(jnp.float32)) + pool_bq).astype(jnp.bfloat16)

    def one_image(image_tokens):
        resid_in = image_tokens.astype(jnp.float32)
        normed = layer_norm(resid_in, ln1_scale, ln1_bias).astype(jnp.bfloat16)
        qkv = (jnp.einsum("nd,dshe->snhe", normed.astype(jnp.float32), w_qkv.astype(jnp.float32)) + b_qkv[:, None]).astype(jnp.bfloat16)
        key_rows = qkv[1].astype(jnp.float32)
        value_rows = qkv[2].astype(jnp.float32)

        def attend_rows(query_rows):
            scores = jnp.einsum("qhe,khe->hqk", query_rows.astype(jnp.float32), key_rows) * score_scale
            weights = jnp.exp(scores - jnp.max(scores, axis=-1, keepdims=True))
            value_sum = jnp.einsum("hqk,khe->hqe", weights.astype(jnp.bfloat16).astype(jnp.float32), value_rows)
            return value_sum / jnp.sum(weights, axis=-1)[:, :, None]

        blocks = lax.map(attend_rows, qkv[0].reshape(TOKENS // ROW_BLOCK, ROW_BLOCK, NUM_HEADS, HEAD_DIM))
        context = blocks.transpose(1, 0, 2, 3).reshape(NUM_HEADS, TOKENS, HEAD_DIM).astype(jnp.bfloat16)
        attn_out = jnp.einsum("hne,hed->nd", context.astype(jnp.float32), w_out.astype(jnp.float32)) + b_out
        resid_mid = (resid_in + attn_out).astype(jnp.bfloat16)
        normed_mid = layer_norm(resid_mid.astype(jnp.float32), ln2_scale, ln2_bias).astype(jnp.bfloat16)
        hidden = jax.nn.gelu(jnp.dot(normed_mid, w_up, preferred_element_type=jnp.float32) + b_up, approximate=True).astype(jnp.bfloat16)
        layer_out = (resid_mid.astype(jnp.float32) + jnp.dot(hidden, w_down, preferred_element_type=jnp.float32) + b_down).astype(jnp.bfloat16)
        tokens_out = layer_norm(layer_out.astype(jnp.float32), lnf_scale, lnf_bias).astype(jnp.bfloat16)
        pool_kv = (jnp.einsum("nd,dshe->snhe", tokens_out.astype(jnp.float32), pool_wkv.astype(jnp.float32)) + pool_bkv[:, None]).astype(jnp.bfloat16)
        pool_scores = jnp.einsum("he,nhe->hn", probe_q.astype(jnp.float32), pool_kv[0].astype(jnp.float32)) * score_scale
        pool_weights = jnp.exp(pool_scores - jnp.max(pool_scores, axis=-1, keepdims=True))
        pool_sum = jnp.einsum("hn,nhe->he", pool_weights.astype(jnp.bfloat16).astype(jnp.float32), pool_kv[1].astype(jnp.float32))
        pooled = (pool_sum / jnp.sum(pool_weights, axis=-1)[:, None]).astype(jnp.bfloat16)
        pooled_out = (jnp.einsum("he,hed->d", pooled.astype(jnp.float32), pool_wout.astype(jnp.float32)) + pool_bout).astype(jnp.bfloat16)
        normed_out = layer_norm(pooled_out.astype(jnp.float32), pool_ln_scale, pool_ln_bias).astype(jnp.bfloat16)
        hidden_out = jax.nn.gelu(jnp.dot(normed_out[None], pool_w_up, preferred_element_type=jnp.float32)[0] + pool_b_up, approximate=True).astype(jnp.bfloat16)
        return pooled_out.astype(jnp.float32) + jnp.dot(hidden_out[None], pool_w_down, preferred_element_type=jnp.float32)[0] + pool_b_down

    return lax.map(one_image, images)
```

```python
import functools
import math

import jax
import jax.numpy as jnp
from jax import lax
from jax.experimental import pallas as pl
from jax.experimental.pallas import tpu as pltpu
from jax.sharding import PartitionSpec as P

EPSILON = 1e-6
LANES = 128
BLOCK = 256
F32 = jnp.float32
BF16 = jnp.bfloat16

(LN1_G, LN1_B, B_OUT, LN2_G, LN2_B, B_DOWN, LNF_G, LNF_B, P_BOUT, P_LN_G, P_LN_B, P_BDOWN, B_Q, B_K, B_V, P_BQ, P_BK, P_BV) = range(18)
N_FIXED = 18
N_SMALL = 17


def layer_norm(values, ln_gain, ln_shift):
    row_mean = jnp.mean(values, axis=-1, keepdims=True)
    centered = values - row_mean
    variance = jnp.mean(centered * centered, axis=-1, keepdims=True)
    return centered * lax.rsqrt(variance + EPSILON) * ln_gain + ln_shift


def gelu(x):
    return jax.nn.gelu(x, approximate=True)


def dot(a, b):
    return lax.dot_general(a, b, (((1,), (0,)), ((), ())), preferred_element_type=F32)


def dot_t(a, b):
    return lax.dot_general(a, b, (((1,), (1,)), ((), ())), preferred_element_type=F32)


def kernel(cfg, images, wqkv_h, wout_h, wup_h, wdown_h, wpkv_h, wpq_h, pwout_h, pwup_h, pwdown_h, *rest):
    n, per, heads, head_dim, width, mlp = cfg
    smalls = rest[:N_SMALL]
    (probe_h, out_ref,
           wqkv, wout, wup, wdown, wpkv, wpq, pwout, pwup, pwdown,
           xbuf, qz, kbuf, vt, s00, s01, s10, s11, p00, p01, p10, p11, mbuf, ctx, hbuf, rbuf, nbuf, hid, zbuf,
           score, pvbuf, ubuf, cols, abuf, gath, vecs, probe, *tail_refs) = rest[N_SMALL:]
    small_bufs = tail_refs[:N_SMALL]
    send_sem, recv_sem, w_sem, gsend_sem, grecv_sem, v_sem = tail_refs[N_SMALL:]
    run = images.shape[1]
    tokens = n * run
    nch = n // 2
    hid_chunks = mlp // width
    pairs = heads // 2
    nq = tokens // BLOCK
    nsteps = pairs * nq
    exp_scale = math.log2(math.e) * head_dim ** -0.5
    me = lax.axis_index("cp")
    own = me // 2
    core = me % 2

    def vec(i):
        return vecs[i:i + 1, :]

    def weight_copy(i, src, dst):
        return pltpu.make_async_copy(src, dst, w_sem.at[i])

    weights = [(wqkv_h, wqkv), (wout_h, wout), (wpq_h, wpq), (wup_h, wup), (wdown_h, wdown), (wpkv_h, wpkv), (pwout_h, pwout), (pwup_h, pwup), (pwdown_h, pwdown)]

    def start_weight(i):
        weight_copy(i, *weights[i]).start()

    def wait_weight(i):
        weight_copy(i, *weights[i]).wait()

    def local_copy(j):
        return pltpu.make_async_copy(images.at[me * per + j], xbuf.at[j, me], recv_sem.at[j, me])

    deltas = [0]
    for d in range(1, nch // 2 + 1):
        deltas.append(d)
        if nch - d != d:
            deltas.append(nch - d)

    def sends(j):
        copies = []
        for delta in deltas:
            for cc in (0, 1):
                if delta == 0 and cc == 0:
                    continue
                dst = ((own + delta) % nch) * 2 + (core + cc) % 2
                copies.append(pltpu.make_async_remote_copy(
                    src_ref=images.at[dst * per + j],
                    dst_ref=xbuf.at[j, me],
                    send_sem=send_sem.at[j, len(copies)],
                    recv_sem=recv_sem.at[j, me],
                    device_id={"cp": dst},
                    device_id_type=pl.DeviceIdType.MESH,
                ))
        return copies

    small_copies = [pltpu.make_async_copy(src, dst, v_sem.at[i]) for i, (src, dst) in enumerate(zip((*smalls, probe_h), (*small_bufs, probe)))]
    start_weight(0)
    for j in range(per):
        local_copy(j).start()
    for copy in small_copies:
        copy.start()

    barrier = pltpu.get_barrier_semaphore()
    for s in range(1, n):
        pl.semaphore_signal(barrier, inc=1, device_id={"cp": (me + s) % n}, device_id_type=pl.DeviceIdType.MESH)
    pl.semaphore_wait(barrier, n - 1)

    for j in range(per):
        for copy in sends(j):
            copy.start()
    for i in range(1, len(weights)):
        start_weight(i)

    for copy in small_copies:
        copy.wait()
    for i, buf in enumerate(small_bufs[:12]):
        vecs[i:i + 1, :] = buf[...].reshape(1, width)
    bqkv_b, pbq_b, pbkv_b, bup_b, pbup_b = small_bufs[12:]
    for h in range(heads):
        lanes = slice(h * head_dim, (h + 1) * head_dim)
        for i, row in enumerate((B_Q, B_K, B_V)):
            vecs[row:row + 1, lanes] = bqkv_b[i, h:h + 1, :]
        vecs[P_BQ:P_BQ + 1, lanes] = pbq_b[h:h + 1, :]
        for i, row in enumerate((P_BK, P_BV)):
            vecs[row:row + 1, lanes] = pbkv_b[h, i:i + 1, :]
    for hc in range(hid_chunks):
        span = slice(hc * width, (hc + 1) * width)
        vecs[N_FIXED + hc:N_FIXED + hc + 1, :] = bup_b[span].reshape(1, width)
        vecs[N_FIXED + hid_chunks + hc:N_FIXED + hid_chunks + hc + 1, :] = pbup_b[span].reshape(1, width)
    for slot, row in enumerate((B_Q, B_V, P_BK)):
        cols[slot] = jnp.transpose(jnp.broadcast_to(vec(row), (LANES, width)))
    qz[...] = jnp.zeros_like(qz)
    abuf[...] = jnp.zeros_like(abuf)
    wait_weight(0)

    def col_bias(slot, lo, size):
        tile = cols[slot, lo:lo + size, :]
        return jnp.concatenate([tile] * (BLOCK // LANES), axis=1)

    def wait_source(j, src):
        pltpu.make_async_copy(images.at[0], xbuf.at[j, src], recv_sem.at[j, src]).wait()

    s_refs = ((s00, s01), (s10, s11))
    p_refs = ((p00, p01), (p10, p11))

    def one_image(j, carry):
        for delta in deltas:
            chip = (own + delta) % nch
            wait_source(j, chip * 2)
            wait_source(j, chip * 2 + 1)
            tok = pl.multiple_of(chip * BLOCK, BLOCK)
            x = xbuf[j, pl.ds(chip * 2, 2)].reshape(BLOCK, width)
            for r0 in range(0, BLOCK, 64):
                hbuf[r0:r0 + 64, :] = layer_norm(x[r0:r0 + 64].astype(F32), vec(LN1_G), vec(LN1_B)).astype(BF16)
            h = hbuf[...]
            kbuf[pl.ds(tok, BLOCK), :] = (dot_t(h, wqkv[width:2 * width, :]) + vec(B_K)).astype(BF16)
            qt = (dot_t(wqkv[0:width, :], h) + col_bias(0, 0, width)).astype(BF16)
            for hd in range(heads):
                off = (hd % 2) * head_dim
                qz[hd, off:off + head_dim, pl.ds(tok, BLOCK)] = qt[hd * head_dim:(hd + 1) * head_dim]
            vt[:, pl.ds(tok, BLOCK)] = (dot_t(wqkv[2 * width:3 * width, :], h) + col_bias(1, 0, width)).astype(BF16)

        def qk(step, slot):
            hp, qb = step // nq, step % nq
            keys = kbuf[:, pl.ds(pl.multiple_of(hp * LANES, LANES), LANES)]
            for hh in (0, 1):
                q = qz[hp * 2 + hh, :, pl.ds(pl.multiple_of(qb * BLOCK, BLOCK), BLOCK)]
                s = dot(keys, q)
                s_refs[slot][hh][...] = s
                mbuf[slot, hh] = jnp.max(s.reshape(tokens // 8, 8, BLOCK), axis=0)

        def softmax_pv(step, slot):
            hp, qb = step // nq, step % nq
            outs = []
            for hh in (0, 1):
                s_ref, p_ref = s_refs[slot][hh], p_refs[slot][hh]
                m = jnp.max(mbuf[slot, hh], axis=0, keepdims=True)
                total = jnp.zeros((8, BLOCK), F32)
                for kc in range(0, tokens, LANES):
                    p = jnp.exp2((s_ref[kc:kc + LANES, :] - m) * exp_scale)
                    total = total + jnp.sum(p.reshape(LANES // 8, 8, BLOCK), axis=0)
                    p_ref[kc:kc + LANES, :] = p.astype(BF16)
                row_sum = jnp.sum(total, axis=0, keepdims=True)
                v = vt[pl.ds(pl.multiple_of(hp * LANES + hh * head_dim, head_dim), head_dim), :]
                outs.append(dot(v, p_ref[...]) * (1.0 / row_sum))
            pair = jnp.transpose(jnp.concatenate(outs, axis=0)).astype(BF16)
            ctx[pl.ds(pl.multiple_of(qb * BLOCK, BLOCK), BLOCK), pl.ds(pl.multiple_of(hp * LANES, LANES), LANES)] = pair

        qk(0, 0)

        def attend(i, c):
            qk(2 * i + 1, 1)
            softmax_pv(2 * i, 0)
            qk((2 * i + 2) % nsteps, 0)
            softmax_pv(2 * i + 1, 1)
            return c

        lax.fori_loop(0, nsteps // 2, attend, 0)

        @pl.when(j == 0)
        def _():
            for i in range(1, 6):
                wait_weight(i)
            q16 = jnp.broadcast_to(probe[...], (16, width))
            u = dot_t(q16, wpq[...]) + vec(P_BQ)
            row = lax.broadcasted_iota(jnp.int32, (16, width), 0)
            col = lax.broadcasted_iota(jnp.int32, (16, width), 1)
            ubuf[...] = jnp.where(col // head_dim == row, u, 0.0).astype(BF16)

        def tail(i, c):
            starts = [pl.multiple_of((2 * i + t) * BLOCK, BLOCK) for t in (0, 1)]

            def resid(t):
                chip = 2 * i + t
                x = xbuf[j, pl.ds(chip * 2, 2)].reshape(BLOCK, width)
                a = dot(ctx[pl.ds(starts[t], BLOCK), :], wout[...])
                rbuf[t] = (x.astype(F32) + a + vec(B_OUT)).astype(BF16)

            def norm(t):
                for r0 in range(0, BLOCK, 64):
                    nbuf[t, r0:r0 + 64, :] = layer_norm(rbuf[t, r0:r0 + 64, :].astype(F32), vec(LN2_G), vec(LN2_B)).astype(BF16)

            def up(t):
                for hc in range(hid_chunks):
                    cols_ = slice(hc * width, (hc + 1) * width)
                    hid[t, :, cols_] = gelu(dot(nbuf[t], wup[:, cols_]) + vec(N_FIXED + hc)).astype(BF16)

            def down(t):
                y = (rbuf[t].astype(F32) + dot(hid[t], wdown[...]) + vec(B_DOWN)).astype(BF16)
                for r0 in range(0, BLOCK, 64):
                    zbuf[t, r0:r0 + 64, :] = layer_norm(y[r0:r0 + 64].astype(F32), vec(LNF_G), vec(LNF_B)).astype(BF16)

            def pool(t):
                z = zbuf[t]
                pk = (dot_t(wpkv[0:width, :], z) + col_bias(2, 0, width)).astype(BF16)
                score[:, pl.ds(starts[t], BLOCK)] = dot(ubuf[...], pk)
                pvbuf[pl.ds(starts[t], BLOCK), :] = (dot_t(z, wpkv[width:2 * width, :]) + vec(P_BV)).astype(BF16)

            resid(0)
            resid(1)
            norm(0)
            up(0)
            norm(1)
            down(0)
            up(1)
            pool(0)
            down(1)
            pool(1)
            return c

        lax.fori_loop(0, nq // 2, tail, 0)

        s = score[...]
        w = jnp.exp2((s - jnp.max(s, axis=-1, keepdims=True)) * exp_scale)
        a = dot(w.astype(BF16), pvbuf[...]) / jnp.sum(w, axis=-1, keepdims=True)
        row = lax.broadcasted_iota(jnp.int32, (16, width), 0)
        col = lax.broadcasted_iota(jnp.int32, (16, width), 1)
        abuf[pl.ds(j, 1), :] = jnp.sum(jnp.where(col // head_dim == row, a, 0.0), axis=0, keepdims=True)
        return carry

    lax.fori_loop(0, per, one_image, 0)

    for i in range(6, len(weights)):
        wait_weight(i)
    o = (dot(abuf[...].astype(BF16), pwout[...]) + vec(P_BOUT)).astype(BF16).astype(F32)
    normed = layer_norm(o, vec(P_LN_G), vec(P_LN_B)).astype(BF16)
    emb = o + vec(P_BDOWN)
    for hc in range(hid_chunks):
        cols_ = slice(hc * width, (hc + 1) * width)
        m = gelu(dot(normed, pwup[:, cols_]) + vec(N_FIXED + hid_chunks + hc)).astype(BF16)
        emb = emb + dot(m, pwdown[cols_, :])
    gath[pl.ds(me, 1)] = emb[0:8][None]

    copies = []
    for s in range(1, n):
        copies.append(pltpu.make_async_remote_copy(
            src_ref=gath.at[me],
            dst_ref=gath.at[me],
            send_sem=gsend_sem.at[s],
            recv_sem=grecv_sem.at[me],
            device_id={"cp": (me + s) % n},
            device_id_type=pl.DeviceIdType.MESH,
        ))
    for copy in copies:
        copy.start()
    for j in range(per):
        for copy in sends(j):
            copy.wait_send()
    for s in range(1, n):
        src = (me + s) % n
        pltpu.make_async_remote_copy(
            src_ref=gath.at[src], dst_ref=gath.at[src], send_sem=gsend_sem.at[s], recv_sem=grecv_sem.at[src],
            device_id={"cp": src}, device_id_type=pl.DeviceIdType.MESH,
        ).wait_recv()
    for copy in copies:
        copy.wait_send()
    for s in range(n):
        out_ref[s * per:(s + 1) * per, :] = gath[s, 0:per, :]


def solution(mesh):
    n = mesh.shape["cp"]

    def device_step(images, ln1_scale, ln1_bias, w_qkv, b_qkv, w_out, b_out, ln2_scale, ln2_bias, w_up, b_up, w_down, b_down, lnf_scale, lnf_bias, pool_probe, pool_wq, pool_bq, pool_wkv, pool_bkv, pool_wout, pool_bout, pool_ln_scale, pool_ln_bias, pool_w_up, pool_b_up, pool_w_down, pool_b_down):
        count, run, width = images.shape
        heads, head_dim = w_qkv.shape[2:]
        mlp = w_up.shape[1]
        per = count // n
        tokens = n * run
        wqkv_t = jnp.transpose(w_qkv, (1, 2, 3, 0)).reshape(3 * width, width)
        wpkv_t = jnp.transpose(pool_wkv, (1, 2, 3, 0)).reshape(2 * width, width)
        wpq_t = jnp.transpose(pool_wq, (1, 2, 0)).reshape(width, width)
        wout2 = w_out.reshape(width, width)
        pwout2 = pool_wout.reshape(width, width)
        smalls = (ln1_scale, ln1_bias, b_out, ln2_scale, ln2_bias, b_down, lnf_scale, lnf_bias, pool_bout, pool_ln_scale, pool_ln_bias, pool_b_down, b_qkv, pool_bq, jnp.transpose(pool_bkv, (1, 0, 2)), b_up, pool_b_up)
        any_spec = pl.BlockSpec(memory_space=pl.ANY)
        vmem_spec = pl.BlockSpec(memory_space=pltpu.VMEM)
        big = (images, wqkv_t, wout2, w_up, w_down, wpkv_t, wpq_t, pwout2, pool_w_up, pool_w_down)
        scratch = [pltpu.VMEM(w.shape, BF16) for w in big[1:]] + [
            pltpu.VMEM((per, n, run, width), BF16),
            pltpu.VMEM((heads, LANES, tokens), BF16),
            pltpu.VMEM((tokens, width), BF16),
            pltpu.VMEM((width, tokens), BF16),
            *[pltpu.VMEM((tokens, BLOCK), F32) for _ in range(4)],
            *[pltpu.VMEM((tokens, BLOCK), BF16) for _ in range(4)],
            pltpu.VMEM((2, 2, 8, BLOCK), F32),
            pltpu.VMEM((tokens, width), BF16),
            pltpu.VMEM((BLOCK, width), BF16),
            pltpu.VMEM((2, BLOCK, width), BF16),
            pltpu.VMEM((2, BLOCK, width), BF16),
            pltpu.VMEM((2, BLOCK, mlp), BF16),
            pltpu.VMEM((2, BLOCK, width), BF16),
            pltpu.VMEM((16, tokens), F32),
            pltpu.VMEM((tokens, width), BF16),
            pltpu.VMEM((16, width), BF16),
            pltpu.VMEM((3, width, LANES), F32),
            pltpu.VMEM((16, width), F32),
            pltpu.VMEM((n, 8, width), F32),
            pltpu.VMEM((N_FIXED + 2 * mlp // width, width), F32),
            pltpu.VMEM(pool_probe.shape, BF16),
            *[pltpu.VMEM(v.shape, F32) for v in smalls],
            pltpu.SemaphoreType.DMA((per, n)),
            pltpu.SemaphoreType.DMA((per, n)),
            pltpu.SemaphoreType.DMA((len(big) - 1,)),
            pltpu.SemaphoreType.DMA((n,)),
            pltpu.SemaphoreType.DMA((n,)),
            pltpu.SemaphoreType.DMA((N_SMALL + 1,)),
        ]
        return pl.pallas_call(
            functools.partial(kernel, (n, per, heads, head_dim, width, mlp)),
            out_shape=jax.ShapeDtypeStruct((count, width), F32),
            in_specs=[any_spec] * (len(big) + len(smalls) + 1),
            out_specs=vmem_spec,
            scratch_shapes=scratch,
            compiler_params=pltpu.CompilerParams(collective_id=0, has_side_effects=True, vmem_limit_bytes=67043328),
            name="encoder_pool",
        )(*big, *smalls, pool_probe)

    in_specs = (P("dp", "cp", None),) + (P(),) * 27
    return jax.shard_map(device_step, mesh=mesh, in_specs=in_specs, out_specs=P("dp", None), check_vma=False)
```

```python
import functools
import math

import jax
import jax.numpy as jnp
from jax import lax
from jax.experimental import pallas as pl
from jax.experimental.pallas import tpu as pltpu
from jax.sharding import PartitionSpec as P

EPSILON = 1e-6
LANES = 128
BLOCK = 256
F32 = jnp.float32
BF16 = jnp.bfloat16

(LN1_G, LN1_B, B_OUT, LN2_G, LN2_B, B_DOWN, LNF_G, LNF_B, P_BOUT, P_LN_G, P_LN_B, P_BDOWN, B_Q, B_K, B_V, P_BQ, P_BK, P_BV) = range(18)
N_FIXED = 18
N_SMALL = 17


def layer_norm(values, ln_gain, ln_shift):
    row_mean = jnp.mean(values, axis=-1, keepdims=True)
    centered = values - row_mean
    variance = jnp.mean(centered * centered, axis=-1, keepdims=True)
    return centered * lax.rsqrt(variance + EPSILON) * ln_gain + ln_shift


def gelu(x):
    return jax.nn.gelu(x, approximate=True)


def dot(a, b):
    return lax.dot_general(a, b, (((1,), (0,)), ((), ())), preferred_element_type=F32)


def dot_t(a, b):
    return lax.dot_general(a, b, (((1,), (1,)), ((), ())), preferred_element_type=F32)


def kernel(cfg, images, wqkv_h, wout_h, wup_h, wdown_h, wpkv_h, wpq_h, pwout_h, pwup_h, pwdown_h, *rest):
    n, per, heads, head_dim, width, mlp = cfg
    smalls = rest[:N_SMALL]
    (probe_h, out_ref,
           wqkv, wout, wup, wdown, wpkv, wpq, pwout, pwup, pwdown,
           xbuf, qz, kbuf, vt, s00, s01, s10, s11, p00, p01, p10, p11, mbuf, ctx, hbuf, rbuf, nbuf, hid, zbuf,
           score, pvbuf, ubuf, cols, abuf, gath, rel, vecs, probe, *tail_refs) = rest[N_SMALL:]
    small_bufs = tail_refs[:N_SMALL]
    send_sem, recv_sem, rel_sem, fwd_sem, w_sem, gsend_sem, grecv_sem, v_sem = tail_refs[N_SMALL:]
    run = images.shape[1]
    tokens = n * run
    nch = n // 2
    hid_chunks = mlp // width
    pairs = heads // 2
    nq = tokens // BLOCK
    nsteps = pairs * nq
    exp_scale = math.log2(math.e) * head_dim ** -0.5
    me = lax.axis_index("cp")
    own = me // 2
    core = me % 2

    def vec(i):
        return vecs[i:i + 1, :]

    def weight_copy(i, src, dst):
        return pltpu.make_async_copy(src, dst, w_sem.at[i])

    weights = [(wqkv_h, wqkv), (wout_h, wout), (wpq_h, wpq), (wup_h, wup), (wdown_h, wdown), (wpkv_h, wpkv), (pwout_h, pwout), (pwup_h, pwup), (pwdown_h, pwdown)]

    def start_weight(i):
        weight_copy(i, *weights[i]).start()

    def wait_weight(i):
        weight_copy(i, *weights[i]).wait()

    def local_copy(j):
        return pltpu.make_async_copy(images.at[me * per + j], xbuf.at[j, me], recv_sem.at[j, me])

    deltas = [0]
    for d in range(1, nch // 2 + 1):
        deltas.append(d)
        if nch - d != d:
            deltas.append(nch - d)

    def remote(src, dst, send, recv, device):
        return pltpu.make_async_remote_copy(
            src_ref=src, dst_ref=dst, send_sem=send, recv_sem=recv, device_id={"cp": device}, device_id_type=pl.DeviceIdType.MESH)

    relayed = nch == 4

    def chip_core(delta, c):
        return ((own + delta + nch) % nch) * 2 + c

    def sends(j):
        copies = []

        def add(block, dst, recv, device):
            copies.append(remote(images.at[block * per + j], dst, send_sem.at[j, len(copies)], recv, device))

        for up in (0, 1) if relayed else ():
            add(chip_core(2, up), rel.at[j, up], rel_sem.at[j, up], chip_core(1 - 2 * up, core))
        for delta in deltas:
            for cc in (0, 1):
                if (delta == 0 and cc == 0) or (relayed and delta == 2):
                    continue
                dst = chip_core(delta, (core + cc) % 2)
                add(dst, xbuf.at[j, me], recv_sem.at[j, me], dst)
        return copies

    def forwards(j):
        copies = []
        for up in (0, 1) if relayed else ():
            source = chip_core(2 * up - 1, core)
            copies.append(remote(rel.at[j, up], xbuf.at[j, source], fwd_sem.at[j, up], recv_sem.at[j, source], chip_core(1 - 2 * up, up)))
        return copies

    def start_forwards(j):
        for up, copy in enumerate(forwards(j)):
            pltpu.make_async_copy(images.at[0], rel.at[j, up], rel_sem.at[j, up]).wait()
            copy.start()

    small_copies = [pltpu.make_async_copy(src, dst, v_sem.at[i]) for i, (src, dst) in enumerate(zip((*smalls, probe_h), (*small_bufs, probe)))]
    start_weight(0)
    for j in range(per):
        local_copy(j).start()
    for copy in small_copies:
        copy.start()

    barrier = pltpu.get_barrier_semaphore()
    for s in range(1, n):
        pl.semaphore_signal(barrier, inc=1, device_id={"cp": (me + s) % n}, device_id_type=pl.DeviceIdType.MESH)
    pl.semaphore_wait(barrier, n - 1)

    for copy in sends(0):
        copy.start()
    for i in range(1, len(weights)):
        start_weight(i)

    for copy in small_copies:
        copy.wait()
    for i, buf in enumerate(small_bufs[:12]):
        vecs[i:i + 1, :] = buf[...].reshape(1, width)
    bqkv_b, pbq_b, pbkv_b, bup_b, pbup_b = small_bufs[12:]
    for h in range(heads):
        lanes = slice(h * head_dim, (h + 1) * head_dim)
        for i, row in enumerate((B_Q, B_K, B_V)):
            vecs[row:row + 1, lanes] = bqkv_b[i, h:h + 1, :]
        vecs[P_BQ:P_BQ + 1, lanes] = pbq_b[h:h + 1, :]
        for i, row in enumerate((P_BK, P_BV)):
            vecs[row:row + 1, lanes] = pbkv_b[h, i:i + 1, :]
    for hc in range(hid_chunks):
        span = slice(hc * width, (hc + 1) * width)
        vecs[N_FIXED + hc:N_FIXED + hc + 1, :] = bup_b[span].reshape(1, width)
        vecs[N_FIXED + hid_chunks + hc:N_FIXED + hid_chunks + hc + 1, :] = pbup_b[span].reshape(1, width)
    for slot, row in enumerate((B_Q, B_V, P_BK)):
        cols[slot] = jnp.transpose(jnp.broadcast_to(vec(row), (LANES, width)))
    qz[...] = jnp.zeros_like(qz)
    abuf[...] = jnp.zeros_like(abuf)
    wait_weight(0)

    def col_bias(slot, lo, size):
        tile = cols[slot, lo:lo + size, :]
        return jnp.concatenate([tile] * (BLOCK // LANES), axis=1)

    def wait_source(j, src):
        pltpu.make_async_copy(images.at[0], xbuf.at[j, src], recv_sem.at[j, src]).wait()

    s_refs = ((s00, s01), (s10, s11))
    p_refs = ((p00, p01), (p10, p11))

    def one_image(j, carry):
        for delta in deltas:
            if delta == 1:
                @pl.when(j == 0)
                def _():
                    start_forwards(0)
                    for later in range(1, per):
                        for copy in sends(later):
                            copy.start()

            chip = (own + delta) % nch
            wait_source(j, chip * 2)
            wait_source(j, chip * 2 + 1)
            tok = pl.multiple_of(chip * BLOCK, BLOCK)
            x = xbuf[j, pl.ds(chip * 2, 2)].reshape(BLOCK, width)
            for r0 in range(0, BLOCK, 64):
                hbuf[r0:r0 + 64, :] = layer_norm(x[r0:r0 + 64].astype(F32), vec(LN1_G), vec(LN1_B)).astype(BF16)
            h = hbuf[...]
            kbuf[pl.ds(tok, BLOCK), :] = (dot_t(h, wqkv[width:2 * width, :]) + vec(B_K)).astype(BF16)
            qt = (dot_t(wqkv[0:width, :], h) + col_bias(0, 0, width)).astype(BF16)
            for hd in range(heads):
                off = (hd % 2) * head_dim
                qz[hd, off:off + head_dim, pl.ds(tok, BLOCK)] = qt[hd * head_dim:(hd + 1) * head_dim]
            vt[:, pl.ds(tok, BLOCK)] = (dot_t(wqkv[2 * width:3 * width, :], h) + col_bias(1, 0, width)).astype(BF16)

        def qk(step, slot):
            hp, qb = step // nq, step % nq
            keys = kbuf[:, pl.ds(pl.multiple_of(hp * LANES, LANES), LANES)]
            for hh in (0, 1):
                q = qz[hp * 2 + hh, :, pl.ds(pl.multiple_of(qb * BLOCK, BLOCK), BLOCK)]
                s = dot(keys, q)
                s_refs[slot][hh][...] = s
                mbuf[slot, hh] = jnp.max(s.reshape(tokens // 8, 8, BLOCK), axis=0)

        def softmax_pv(step, slot):
            hp, qb = step // nq, step % nq
            outs = []
            for hh in (0, 1):
                s_ref, p_ref = s_refs[slot][hh], p_refs[slot][hh]
                m = jnp.max(mbuf[slot, hh], axis=0, keepdims=True)
                total = jnp.zeros((8, BLOCK), F32)
                for kc in range(0, tokens, LANES):
                    p = jnp.exp2((s_ref[kc:kc + LANES, :] - m) * exp_scale)
                    total = total + jnp.sum(p.reshape(LANES // 8, 8, BLOCK), axis=0)
                    p_ref[kc:kc + LANES, :] = p.astype(BF16)
                row_sum = jnp.sum(total, axis=0, keepdims=True)
                v = vt[pl.ds(pl.multiple_of(hp * LANES + hh * head_dim, head_dim), head_dim), :]
                outs.append(dot(v, p_ref[...]) * (1.0 / row_sum))
            pair = jnp.transpose(jnp.concatenate(outs, axis=0)).astype(BF16)
            ctx[pl.ds(pl.multiple_of(qb * BLOCK, BLOCK), BLOCK), pl.ds(pl.multiple_of(hp * LANES, LANES), LANES)] = pair

        qk(0, 0)

        def attend(i, c):
            qk(2 * i + 1, 1)
            softmax_pv(2 * i, 0)
            qk((2 * i + 2) % nsteps, 0)
            softmax_pv(2 * i + 1, 1)
            return c

        lax.fori_loop(0, nsteps // 2, attend, 0)

        @pl.when(j == 0)
        def _():
            for later in range(1, per):
                start_forwards(later)
            for i in range(1, 6):
                wait_weight(i)
            q16 = jnp.broadcast_to(probe[...], (16, width))
            u = dot_t(q16, wpq[...]) + vec(P_BQ)
            row = lax.broadcasted_iota(jnp.int32, (16, width), 0)
            col = lax.broadcasted_iota(jnp.int32, (16, width), 1)
            ubuf[...] = jnp.where(col // head_dim == row, u, 0.0).astype(BF16)

        def tail(i, c):
            starts = [pl.multiple_of((2 * i + t) * BLOCK, BLOCK) for t in (0, 1)]

            def resid(t):
                chip = 2 * i + t
                x = xbuf[j, pl.ds(chip * 2, 2)].reshape(BLOCK, width)
                a = dot(ctx[pl.ds(starts[t], BLOCK), :], wout[...])
                rbuf[t] = (x.astype(F32) + a + vec(B_OUT)).astype(BF16)

            def norm(t):
                for r0 in range(0, BLOCK, 64):
                    nbuf[t, r0:r0 + 64, :] = layer_norm(rbuf[t, r0:r0 + 64, :].astype(F32), vec(LN2_G), vec(LN2_B)).astype(BF16)

            def up(t):
                for hc in range(hid_chunks):
                    cols_ = slice(hc * width, (hc + 1) * width)
                    hid[t, :, cols_] = gelu(dot(nbuf[t], wup[:, cols_]) + vec(N_FIXED + hc)).astype(BF16)

            def down(t):
                y = (rbuf[t].astype(F32) + dot(hid[t], wdown[...]) + vec(B_DOWN)).astype(BF16)
                for r0 in range(0, BLOCK, 64):
                    zbuf[t, r0:r0 + 64, :] = layer_norm(y[r0:r0 + 64].astype(F32), vec(LNF_G), vec(LNF_B)).astype(BF16)

            def pool(t):
                z = zbuf[t]
                pk = (dot_t(wpkv[0:width, :], z) + col_bias(2, 0, width)).astype(BF16)
                score[:, pl.ds(starts[t], BLOCK)] = dot(ubuf[...], pk)
                pvbuf[pl.ds(starts[t], BLOCK), :] = (dot_t(z, wpkv[width:2 * width, :]) + vec(P_BV)).astype(BF16)

            resid(0)
            resid(1)
            norm(0)
            up(0)
            norm(1)
            down(0)
            up(1)
            pool(0)
            down(1)
            pool(1)
            return c

        lax.fori_loop(0, nq // 2, tail, 0)

        s = score[...]
        w = jnp.exp2((s - jnp.max(s, axis=-1, keepdims=True)) * exp_scale)
        a = dot(w.astype(BF16), pvbuf[...]) / jnp.sum(w, axis=-1, keepdims=True)
        row = lax.broadcasted_iota(jnp.int32, (16, width), 0)
        col = lax.broadcasted_iota(jnp.int32, (16, width), 1)
        abuf[pl.ds(j, 1), :] = jnp.sum(jnp.where(col // head_dim == row, a, 0.0), axis=0, keepdims=True)
        return carry

    lax.fori_loop(0, per, one_image, 0)

    for i in range(6, len(weights)):
        wait_weight(i)
    o = (dot(abuf[...].astype(BF16), pwout[...]) + vec(P_BOUT)).astype(BF16).astype(F32)
    normed = layer_norm(o, vec(P_LN_G), vec(P_LN_B)).astype(BF16)
    emb = o + vec(P_BDOWN)
    for hc in range(hid_chunks):
        cols_ = slice(hc * width, (hc + 1) * width)
        m = gelu(dot(normed, pwup[:, cols_]) + vec(N_FIXED + hid_chunks + hc)).astype(BF16)
        emb = emb + dot(m, pwdown[cols_, :])
    gath[pl.ds(me, 1)] = emb[0:8][None]

    copies = []
    for s in range(1, n):
        copies.append(pltpu.make_async_remote_copy(
            src_ref=gath.at[me],
            dst_ref=gath.at[me],
            send_sem=gsend_sem.at[s],
            recv_sem=grecv_sem.at[me],
            device_id={"cp": (me + s) % n},
            device_id_type=pl.DeviceIdType.MESH,
        ))
    for copy in copies:
        copy.start()
    for j in range(per):
        for copy in sends(j) + forwards(j):
            copy.wait_send()
    for s in range(1, n):
        src = (me + s) % n
        pltpu.make_async_remote_copy(
            src_ref=gath.at[src], dst_ref=gath.at[src], send_sem=gsend_sem.at[s], recv_sem=grecv_sem.at[src],
            device_id={"cp": src}, device_id_type=pl.DeviceIdType.MESH,
        ).wait_recv()
    for copy in copies:
        copy.wait_send()
    for s in range(n):
        out_ref[s * per:(s + 1) * per, :] = gath[s, 0:per, :]


def solution(mesh):
    n = mesh.shape["cp"]

    def device_step(images, ln1_scale, ln1_bias, w_qkv, b_qkv, w_out, b_out, ln2_scale, ln2_bias, w_up, b_up, w_down, b_down, lnf_scale, lnf_bias, pool_probe, pool_wq, pool_bq, pool_wkv, pool_bkv, pool_wout, pool_bout, pool_ln_scale, pool_ln_bias, pool_w_up, pool_b_up, pool_w_down, pool_b_down):
        count, run, width = images.shape
        heads, head_dim = w_qkv.shape[2:]
        mlp = w_up.shape[1]
        per = count // n
        tokens = n * run
        wqkv_t = jnp.transpose(w_qkv, (1, 2, 3, 0)).reshape(3 * width, width)
        wpkv_t = jnp.transpose(pool_wkv, (1, 2, 3, 0)).reshape(2 * width, width)
        wpq_t = jnp.transpose(pool_wq, (1, 2, 0)).reshape(width, width)
        wout2 = w_out.reshape(width, width)
        pwout2 = pool_wout.reshape(width, width)
        smalls = (ln1_scale, ln1_bias, b_out, ln2_scale, ln2_bias, b_down, lnf_scale, lnf_bias, pool_bout, pool_ln_scale, pool_ln_bias, pool_b_down, b_qkv, pool_bq, jnp.transpose(pool_bkv, (1, 0, 2)), b_up, pool_b_up)
        any_spec = pl.BlockSpec(memory_space=pl.ANY)
        vmem_spec = pl.BlockSpec(memory_space=pltpu.VMEM)
        big = (images, wqkv_t, wout2, w_up, w_down, wpkv_t, wpq_t, pwout2, pool_w_up, pool_w_down)
        scratch = [pltpu.VMEM(w.shape, BF16) for w in big[1:]] + [
            pltpu.VMEM((per, n, run, width), BF16),
            pltpu.VMEM((heads, LANES, tokens), BF16),
            pltpu.VMEM((tokens, width), BF16),
            pltpu.VMEM((width, tokens), BF16),
            *[pltpu.VMEM((tokens, BLOCK), F32) for _ in range(4)],
            *[pltpu.VMEM((tokens, BLOCK), BF16) for _ in range(4)],
            pltpu.VMEM((2, 2, 8, BLOCK), F32),
            pltpu.VMEM((tokens, width), BF16),
            pltpu.VMEM((BLOCK, width), BF16),
            pltpu.VMEM((2, BLOCK, width), BF16),
            pltpu.VMEM((2, BLOCK, width), BF16),
            pltpu.VMEM((2, BLOCK, mlp), BF16),
            pltpu.VMEM((2, BLOCK, width), BF16),
            pltpu.VMEM((16, tokens), F32),
            pltpu.VMEM((tokens, width), BF16),
            pltpu.VMEM((16, width), BF16),
            pltpu.VMEM((3, width, LANES), F32),
            pltpu.VMEM((16, width), F32),
            pltpu.VMEM((n, 8, width), F32),
            pltpu.VMEM((per, 2, run, width), BF16),
            pltpu.VMEM((N_FIXED + 2 * mlp // width, width), F32),
            pltpu.VMEM(pool_probe.shape, BF16),
            *[pltpu.VMEM(v.shape, F32) for v in smalls],
            pltpu.SemaphoreType.DMA((per, n)),
            pltpu.SemaphoreType.DMA((per, n)),
            pltpu.SemaphoreType.DMA((per, 2)),
            pltpu.SemaphoreType.DMA((per, 2)),
            pltpu.SemaphoreType.DMA((len(big) - 1,)),
            pltpu.SemaphoreType.DMA((n,)),
            pltpu.SemaphoreType.DMA((n,)),
            pltpu.SemaphoreType.DMA((N_SMALL + 1,)),
        ]
        return pl.pallas_call(
            functools.partial(kernel, (n, per, heads, head_dim, width, mlp)),
            out_shape=jax.ShapeDtypeStruct((count, width), F32),
            in_specs=[any_spec] * (len(big) + len(smalls) + 1),
            out_specs=vmem_spec,
            scratch_shapes=scratch,
            compiler_params=pltpu.CompilerParams(collective_id=0, has_side_effects=True, vmem_limit_bytes=67043328),
            name="encoder_pool",
        )(*big, *smalls, pool_probe)

    in_specs = (P("dp", "cp", None),) + (P(),) * 27
    return jax.shard_map(device_step, mesh=mesh, in_specs=in_specs, out_specs=P("dp", None), check_vma=False)
```

```python
import functools
import math

import jax
import jax.numpy as jnp
from jax import lax
from jax.experimental import pallas as pl
from jax.experimental.pallas import tpu as pltpu
from jax.sharding import PartitionSpec as P

EPSILON = 1e-6
LANES = 128
BLOCK = 256
UNROLL = 4
F32 = jnp.float32
BF16 = jnp.bfloat16

(LN1_G, LN1_B, B_OUT, LN2_G, LN2_B, B_DOWN, LNF_G, LNF_B, P_BOUT, P_LN_G, P_LN_B, P_BDOWN, B_Q, B_K, B_V, P_BQ, P_BK, P_BV) = range(18)
N_FIXED = 18
N_SMALL = 17


def layer_norm(values, ln_gain, ln_shift):
    row_mean = jnp.mean(values, axis=-1, keepdims=True)
    centered = values - row_mean
    variance = jnp.mean(centered * centered, axis=-1, keepdims=True)
    return centered * lax.rsqrt(variance + EPSILON) * ln_gain + ln_shift


def gelu(x):
    return jax.nn.gelu(x, approximate=True)


def dot(a, b):
    return lax.dot_general(a, b, (((1,), (0,)), ((), ())), preferred_element_type=F32)


def dot_t(a, b):
    return lax.dot_general(a, b, (((1,), (1,)), ((), ())), preferred_element_type=F32)


def halves_t(a_ref, lo, size, b):
    half = size // 2
    return [(r, half, dot_t(a_ref[lo + r:lo + r + half, :], b)) for r in (0, half)]


def kernel(cfg, images, wqkv_h, wout_h, wup_h, wdown_h, wpkv_h, wpq_h, pwout_h, pwup_h, pwdown_h, *rest):
    n, per, heads, head_dim, width, mlp = cfg
    smalls = rest[:N_SMALL]
    (probe_h, out_ref,
           wqkv, wout, wup, wdown, wpkv, wpq, pwout, pwup, pwdown,
           xbuf, qz, kbuf, vt, s00, s01, s10, s11, p00, p01, p10, p11, mbuf, ctx, hbuf, rbuf, nbuf, hid, zbuf,
           score, pvbuf, ubuf, cols, abuf, gath, rel, vecs, probe, *tail_refs) = rest[N_SMALL:]
    small_bufs = tail_refs[:N_SMALL]
    send_sem, recv_sem, rel_sem, fwd_sem, w_sem, gsend_sem, grecv_sem, v_sem = tail_refs[N_SMALL:]
    run = images.shape[1]
    tokens = n * run
    nch = n // 2
    hid_chunks = mlp // width
    pairs = heads // 2
    nq = tokens // BLOCK
    nsteps = pairs * nq
    exp_scale = math.log2(math.e) * head_dim ** -0.5
    me = lax.axis_index("cp")
    own = me // 2
    core = me % 2

    def vec(i):
        return vecs[i:i + 1, :]

    def weight_copy(i, src, dst):
        return pltpu.make_async_copy(src, dst, w_sem.at[i])

    weights = [(wqkv_h, wqkv), (wout_h, wout), (wpq_h, wpq), (wup_h, wup), (wdown_h, wdown), (wpkv_h, wpkv), (pwout_h, pwout), (pwup_h, pwup), (pwdown_h, pwdown)]

    def start_weight(i):
        weight_copy(i, *weights[i]).start()

    def wait_weight(i):
        weight_copy(i, *weights[i]).wait()

    def local_copy(j):
        return pltpu.make_async_copy(images.at[me * per + j], xbuf.at[j, me], recv_sem.at[j, me])

    deltas = [0]
    for d in range(1, nch // 2 + 1):
        deltas.append(d)
        if nch - d != d:
            deltas.append(nch - d)

    def remote(src, dst, send, recv, device):
        return pltpu.make_async_remote_copy(
            src_ref=src, dst_ref=dst, send_sem=send, recv_sem=recv, device_id={"cp": device}, device_id_type=pl.DeviceIdType.MESH)

    relayed = nch == 4

    def chip_core(delta, c):
        return ((own + delta + nch) % nch) * 2 + c

    def sends(j):
        copies = []

        def add(block, dst, recv, device):
            copies.append(remote(images.at[block * per + j], dst, send_sem.at[j, len(copies)], recv, device))

        for up in (0, 1) if relayed else ():
            add(chip_core(2, up), rel.at[j, up], rel_sem.at[j, up], chip_core(1 - 2 * up, core))
        for delta in deltas:
            for cc in (0, 1):
                if (delta == 0 and cc == 0) or (relayed and delta == 2):
                    continue
                dst = chip_core(delta, (core + cc) % 2)
                add(dst, xbuf.at[j, me], recv_sem.at[j, me], dst)
        return copies

    def forwards(j):
        copies = []
        for up in (0, 1) if relayed else ():
            source = chip_core(2 * up - 1, core)
            copies.append(remote(rel.at[j, up], xbuf.at[j, source], fwd_sem.at[j, up], recv_sem.at[j, source], chip_core(1 - 2 * up, up)))
        return copies

    def start_forwards(j):
        for up, copy in enumerate(forwards(j)):
            pltpu.make_async_copy(images.at[0], rel.at[j, up], rel_sem.at[j, up]).wait()
            copy.start()

    small_copies = [pltpu.make_async_copy(src, dst, v_sem.at[i]) for i, (src, dst) in enumerate(zip((*smalls, probe_h), (*small_bufs, probe)))]
    start_weight(0)
    for j in range(per):
        local_copy(j).start()
    for copy in small_copies:
        copy.start()

    barrier = pltpu.get_barrier_semaphore()
    for s in range(1, n):
        pl.semaphore_signal(barrier, inc=1, device_id={"cp": (me + s) % n}, device_id_type=pl.DeviceIdType.MESH)
    pl.semaphore_wait(barrier, n - 1)

    for copy in sends(0):
        copy.start()
    for i in range(1, len(weights)):
        start_weight(i)

    for copy in small_copies:
        copy.wait()
    for i, buf in enumerate(small_bufs[:12]):
        vecs[i:i + 1, :] = buf[...].reshape(1, width)
    bqkv_b, pbq_b, pbkv_b, bup_b, pbup_b = small_bufs[12:]
    for h in range(heads):
        lanes = slice(h * head_dim, (h + 1) * head_dim)
        for i, row in enumerate((B_Q, B_K, B_V)):
            vecs[row:row + 1, lanes] = bqkv_b[i, h:h + 1, :]
        vecs[P_BQ:P_BQ + 1, lanes] = pbq_b[h:h + 1, :]
        for i, row in enumerate((P_BK, P_BV)):
            vecs[row:row + 1, lanes] = pbkv_b[h, i:i + 1, :]
    for hc in range(hid_chunks):
        span = slice(hc * width, (hc + 1) * width)
        vecs[N_FIXED + hc:N_FIXED + hc + 1, :] = bup_b[span].reshape(1, width)
        vecs[N_FIXED + hid_chunks + hc:N_FIXED + hid_chunks + hc + 1, :] = pbup_b[span].reshape(1, width)
    for slot, row in enumerate((B_Q, B_V, P_BK)):
        cols[slot] = jnp.transpose(jnp.broadcast_to(vec(row), (LANES, width)))
    qz[...] = jnp.zeros_like(qz)
    abuf[...] = jnp.zeros_like(abuf)
    wait_weight(0)

    def col_bias(slot, lo, size):
        tile = cols[slot, lo:lo + size, :]
        return jnp.concatenate([tile] * (BLOCK // LANES), axis=1)

    def wait_source(j, src):
        pltpu.make_async_copy(images.at[0], xbuf.at[j, src], recv_sem.at[j, src]).wait()

    s_refs = ((s00, s01), (s10, s11))
    p_refs = ((p00, p01), (p10, p11))

    def one_image(j, carry):
        def chip_of(k):
            return (own + deltas[k]) % nch

        def enter(k):
            x = xbuf[j, pl.ds(chip_of(k) * 2, 2)].reshape(BLOCK, width)
            for r0 in range(0, BLOCK, 64):
                hbuf[k % 2, r0:r0 + 64, :] = layer_norm(x[r0:r0 + 64].astype(F32), vec(LN1_G), vec(LN1_B)).astype(BF16)

        def project(k):
            tok = pl.multiple_of(chip_of(k) * BLOCK, BLOCK)
            h = hbuf[k % 2]
            for r, size, qt in halves_t(wqkv, 0, width, h):
                qt = (qt + col_bias(0, r, size)).astype(BF16)
                for h0 in range(0, size, head_dim):
                    hd = (r + h0) // head_dim
                    off = (hd % 2) * head_dim
                    qz[hd, off:off + head_dim, pl.ds(tok, BLOCK)] = qt[h0:h0 + head_dim]
            for r, size, v in halves_t(wqkv, 2 * width, width, h):
                vt[r:r + size, pl.ds(tok, BLOCK)] = (v + col_bias(1, r, size)).astype(BF16)
            kbuf[pl.ds(tok, BLOCK), :] = (dot_t(h, wqkv[width:2 * width, :]) + vec(B_K)).astype(BF16)

        def wait_chip(k):
            wait_source(j, chip_of(k) * 2)
            wait_source(j, chip_of(k) * 2 + 1)

        @pl.when(j == 0)
        def _():
            for k in range(nch):
                if k == 1:
                    start_forwards(0)
                    for later in range(1, per):
                        for copy in sends(later):
                            copy.start()
                wait_chip(k)
                enter(k)
                project(k)

        @pl.when(j > 0)
        def _():
            for k in range(nch):
                wait_chip(k)
            enter(0)
            for k in range(nch):
                if k + 1 < nch:
                    enter(k + 1)
                project(k)

        def qk(step, slot):
            hp, qb = step // nq, step % nq
            keys = kbuf[:, pl.ds(pl.multiple_of(hp * LANES, LANES), LANES)]
            for hh in (0, 1):
                q = qz[hp * 2 + hh, :, pl.ds(pl.multiple_of(qb * BLOCK, BLOCK), BLOCK)]
                s = dot(keys, q)
                s_refs[slot][hh][...] = s
                mbuf[slot, hh] = jnp.max(s.reshape(tokens // 8, 8, BLOCK), axis=0)

        def softmax_pv(step, slot):
            hp, qb = step // nq, step % nq
            outs = []
            for hh in (0, 1):
                s_ref, p_ref = s_refs[slot][hh], p_refs[slot][hh]
                m = jnp.max(mbuf[slot, hh], axis=0, keepdims=True)
                total = jnp.zeros((8, BLOCK), F32)
                for kc in range(0, tokens, LANES):
                    p = jnp.exp2((s_ref[kc:kc + LANES, :] - m) * exp_scale)
                    total = total + jnp.sum(p.reshape(LANES // 8, 8, BLOCK), axis=0)
                    p_ref[kc:kc + LANES, :] = p.astype(BF16)
                row_sum = jnp.sum(total, axis=0, keepdims=True)
                v = vt[pl.ds(pl.multiple_of(hp * LANES + hh * head_dim, head_dim), head_dim), :]
                outs.append(dot(v, p_ref[...]) * (1.0 / row_sum))
            pair = jnp.transpose(jnp.concatenate(outs, axis=0)).astype(BF16)
            ctx[pl.ds(pl.multiple_of(qb * BLOCK, BLOCK), BLOCK), pl.ds(pl.multiple_of(hp * LANES, LANES), LANES)] = pair

        qk(0, 0)

        def attend(i, c):
            for k in range(UNROLL):
                qk((UNROLL * i + k + 1) % nsteps, (k + 1) % 2)
                softmax_pv(UNROLL * i + k, k % 2)
            return c

        lax.fori_loop(0, nsteps // UNROLL, attend, 0)

        @pl.when(j == 0)
        def _():
            for later in range(1, per):
                start_forwards(later)
            for i in range(1, 6):
                wait_weight(i)
            q16 = jnp.broadcast_to(probe[...], (16, width))
            u = dot_t(q16, wpq[...]) + vec(P_BQ)
            row = lax.broadcasted_iota(jnp.int32, (16, width), 0)
            col = lax.broadcasted_iota(jnp.int32, (16, width), 1)
            ubuf[...] = jnp.where(col // head_dim == row, u, 0.0).astype(BF16)

        def pool(t, block):
            z = zbuf[t]
            start = pl.multiple_of((block % nq) * BLOCK, BLOCK)
            parts = [(pk + col_bias(2, r, size)).astype(BF16) for r, size, pk in halves_t(wpkv, 0, width, z)]
            score[:, pl.ds(start, BLOCK)] = dot(ubuf[...], jnp.concatenate(parts, axis=0))
            pvbuf[pl.ds(start, BLOCK), :] = (dot_t(z, wpkv[width:2 * width, :]) + vec(P_BV)).astype(BF16)

        def tail(i, c):
            starts = [pl.multiple_of((2 * i + t) * BLOCK, BLOCK) for t in (0, 1)]

            def resid(t):
                chip = 2 * i + t
                x = xbuf[j, pl.ds(chip * 2, 2)].reshape(BLOCK, width)
                a = dot(ctx[pl.ds(starts[t], BLOCK), :], wout[...])
                rbuf[t] = (x.astype(F32) + a + vec(B_OUT)).astype(BF16)

            def norm(t):
                for r0 in range(0, BLOCK, 64):
                    nbuf[t, r0:r0 + 64, :] = layer_norm(rbuf[t, r0:r0 + 64, :].astype(F32), vec(LN2_G), vec(LN2_B)).astype(BF16)

            def up(t):
                for hc in range(hid_chunks):
                    cols_ = slice(hc * width, (hc + 1) * width)
                    hid[t, :, cols_] = gelu(dot(nbuf[t], wup[:, cols_]) + vec(N_FIXED + hc)).astype(BF16)

            def down(t):
                y = (rbuf[t].astype(F32) + dot(hid[t], wdown[...]) + vec(B_DOWN)).astype(BF16)
                for r0 in range(0, BLOCK, 64):
                    zbuf[t, r0:r0 + 64, :] = layer_norm(y[r0:r0 + 64].astype(F32), vec(LNF_G), vec(LNF_B)).astype(BF16)

            resid(0)
            resid(1)
            pool(1, 2 * i + nq - 1)
            norm(0)
            up(0)
            norm(1)
            down(0)
            up(1)
            pool(0, 2 * i)
            down(1)
            return c

        zbuf[1] = jnp.zeros((BLOCK, width), BF16)
        lax.fori_loop(0, nq // 2, tail, 0)
        pool(1, nq - 1)

        s = score[...]
        w = jnp.exp2((s - jnp.max(s, axis=-1, keepdims=True)) * exp_scale)
        a = dot(w.astype(BF16), pvbuf[...]) / jnp.sum(w, axis=-1, keepdims=True)
        row = lax.broadcasted_iota(jnp.int32, (16, width), 0)
        col = lax.broadcasted_iota(jnp.int32, (16, width), 1)
        abuf[pl.ds(j, 1), :] = jnp.sum(jnp.where(col // head_dim == row, a, 0.0), axis=0, keepdims=True)
        return carry

    lax.fori_loop(0, per, one_image, 0)

    for i in range(6, len(weights)):
        wait_weight(i)
    o = (dot(abuf[...].astype(BF16), pwout[...]) + vec(P_BOUT)).astype(BF16).astype(F32)
    normed = layer_norm(o, vec(P_LN_G), vec(P_LN_B)).astype(BF16)
    emb = o + vec(P_BDOWN)
    for hc in range(hid_chunks):
        cols_ = slice(hc * width, (hc + 1) * width)
        m = gelu(dot(normed, pwup[:, cols_]) + vec(N_FIXED + hid_chunks + hc)).astype(BF16)
        emb = emb + dot(m, pwdown[cols_, :])
    gath[pl.ds(me, 1)] = emb[0:8][None]

    copies = []
    for s in range(1, n):
        copies.append(pltpu.make_async_remote_copy(
            src_ref=gath.at[me],
            dst_ref=gath.at[me],
            send_sem=gsend_sem.at[s],
            recv_sem=grecv_sem.at[me],
            device_id={"cp": (me + s) % n},
            device_id_type=pl.DeviceIdType.MESH,
        ))
    for copy in copies:
        copy.start()
    for j in range(per):
        for copy in sends(j) + forwards(j):
            copy.wait_send()
    for s in range(1, n):
        src = (me + s) % n
        pltpu.make_async_remote_copy(
            src_ref=gath.at[src], dst_ref=gath.at[src], send_sem=gsend_sem.at[s], recv_sem=grecv_sem.at[src],
            device_id={"cp": src}, device_id_type=pl.DeviceIdType.MESH,
        ).wait_recv()
    for copy in copies:
        copy.wait_send()
    for s in range(n):
        out_ref[s * per:(s + 1) * per, :] = gath[s, 0:per, :]


def solution(mesh):
    n = mesh.shape["cp"]

    def device_step(images, ln1_scale, ln1_bias, w_qkv, b_qkv, w_out, b_out, ln2_scale, ln2_bias, w_up, b_up, w_down, b_down, lnf_scale, lnf_bias, pool_probe, pool_wq, pool_bq, pool_wkv, pool_bkv, pool_wout, pool_bout, pool_ln_scale, pool_ln_bias, pool_w_up, pool_b_up, pool_w_down, pool_b_down):
        count, run, width = images.shape
        heads, head_dim = w_qkv.shape[2:]
        mlp = w_up.shape[1]
        per = count // n
        tokens = n * run
        wqkv_t = jnp.transpose(w_qkv, (1, 2, 3, 0)).reshape(3 * width, width)
        wpkv_t = jnp.transpose(pool_wkv, (1, 2, 3, 0)).reshape(2 * width, width)
        wpq_t = jnp.transpose(pool_wq, (1, 2, 0)).reshape(width, width)
        wout2 = w_out.reshape(width, width)
        pwout2 = pool_wout.reshape(width, width)
        smalls = (ln1_scale, ln1_bias, b_out, ln2_scale, ln2_bias, b_down, lnf_scale, lnf_bias, pool_bout, pool_ln_scale, pool_ln_bias, pool_b_down, b_qkv, pool_bq, jnp.transpose(pool_bkv, (1, 0, 2)), b_up, pool_b_up)
        any_spec = pl.BlockSpec(memory_space=pl.ANY)
        vmem_spec = pl.BlockSpec(memory_space=pltpu.VMEM)
        big = (images, wqkv_t, wout2, w_up, w_down, wpkv_t, wpq_t, pwout2, pool_w_up, pool_w_down)
        scratch = [pltpu.VMEM(w.shape, BF16) for w in big[1:]] + [
            pltpu.VMEM((per, n, run, width), BF16),
            pltpu.VMEM((heads, LANES, tokens), BF16),
            pltpu.VMEM((tokens, width), BF16),
            pltpu.VMEM((width, tokens), BF16),
            *[pltpu.VMEM((tokens, BLOCK), F32) for _ in range(4)],
            *[pltpu.VMEM((tokens, BLOCK), BF16) for _ in range(4)],
            pltpu.VMEM((2, 2, 8, BLOCK), F32),
            pltpu.VMEM((tokens, width), BF16),
            pltpu.VMEM((2, BLOCK, width), BF16),
            pltpu.VMEM((2, BLOCK, width), BF16),
            pltpu.VMEM((2, BLOCK, width), BF16),
            pltpu.VMEM((2, BLOCK, mlp), BF16),
            pltpu.VMEM((2, BLOCK, width), BF16),
            pltpu.VMEM((16, tokens), F32),
            pltpu.VMEM((tokens, width), BF16),
            pltpu.VMEM((16, width), BF16),
            pltpu.VMEM((3, width, LANES), F32),
            pltpu.VMEM((16, width), F32),
            pltpu.VMEM((n, 8, width), F32),
            pltpu.VMEM((per, 2, run, width), BF16),
            pltpu.VMEM((N_FIXED + 2 * mlp // width, width), F32),
            pltpu.VMEM(pool_probe.shape, BF16),
            *[pltpu.VMEM(v.shape, F32) for v in smalls],
            pltpu.SemaphoreType.DMA((per, n)),
            pltpu.SemaphoreType.DMA((per, n)),
            pltpu.SemaphoreType.DMA((per, 2)),
            pltpu.SemaphoreType.DMA((per, 2)),
            pltpu.SemaphoreType.DMA((len(big) - 1,)),
            pltpu.SemaphoreType.DMA((n,)),
            pltpu.SemaphoreType.DMA((n,)),
            pltpu.SemaphoreType.DMA((N_SMALL + 1,)),
        ]
        return pl.pallas_call(
            functools.partial(kernel, (n, per, heads, head_dim, width, mlp)),
            out_shape=jax.ShapeDtypeStruct((count, width), F32),
            in_specs=[any_spec] * (len(big) + len(smalls) + 1),
            out_specs=vmem_spec,
            scratch_shapes=scratch,
            compiler_params=pltpu.CompilerParams(collective_id=0, has_side_effects=True, vmem_limit_bytes=67043328),
            name="encoder_pool",
        )(*big, *smalls, pool_probe)

    in_specs = (P("dp", "cp", None),) + (P(),) * 27
    return jax.shard_map(device_step, mesh=mesh, in_specs=in_specs, out_specs=P("dp", None), check_vma=False)
```

```python
import functools
import math

import jax
import jax.numpy as jnp
from jax import lax
from jax.experimental import pallas as pl
from jax.experimental.pallas import tpu as pltpu
from jax.sharding import PartitionSpec as P

EPSILON = 1e-6
LANES = 128
BLOCK = 256
UNROLL = 4
F32 = jnp.float32
BF16 = jnp.bfloat16

(LN1_G, LN1_B, B_OUT, LN2_G, LN2_B, B_DOWN, LNF_G, LNF_B, P_BOUT, P_LN_G, P_LN_B, P_BDOWN, B_Q, B_K, B_V, P_BQ, P_BK, P_BV) = range(18)
N_FIXED = 18
N_SMALL = 17


def layer_norm(values, ln_gain, ln_shift):
    row_mean = jnp.mean(values, axis=-1, keepdims=True)
    centered = values - row_mean
    variance = jnp.mean(centered * centered, axis=-1, keepdims=True)
    return centered * lax.rsqrt(variance + EPSILON) * ln_gain + ln_shift


def gelu(x):
    return jax.nn.gelu(x, approximate=True)


def dot(a, b):
    return lax.dot_general(a, b, (((1,), (0,)), ((), ())), preferred_element_type=F32)


def dot_t(a, b):
    return lax.dot_general(a, b, (((1,), (1,)), ((), ())), preferred_element_type=F32)


def halves_t(a_ref, lo, size, b):
    half = size // 2
    return [(r, half, dot_t(a_ref[lo + r:lo + r + half, :], b)) for r in (0, half)]


def kernel(cfg, images, wqkv_h, wout_h, wup_h, wdown_h, wpkv_h, wpq_h, pwout_h, pwup_h, pwdown_h, *rest):
    n, per, heads, head_dim, width, mlp = cfg
    smalls = rest[:N_SMALL]
    (probe_h, out_ref,
           wqkv, wout, wup, wdown, wpkv, wpq, pwout, pwup, pwdown,
           xbuf, qz, kbuf, vt, s00, s01, s10, s11, p00, p01, p10, p11, mbuf, ctx, hbuf, rbuf, nbuf, hid, zbuf,
           score, pvbuf, ubuf, cols, abuf, gath, rel, vecs, probe, *tail_refs) = rest[N_SMALL:]
    small_bufs = tail_refs[:N_SMALL]
    send_sem, recv_sem, rel_sem, fwd_sem, w_sem, gsend_sem, grecv_sem, v_sem = tail_refs[N_SMALL:]
    run = images.shape[1]
    tokens = n * run
    nch = n // 2
    hid_chunks = mlp // width
    pairs = heads // 2
    nq = tokens // BLOCK
    nsteps = pairs * nq
    exp_scale = math.log2(math.e) * head_dim ** -0.5
    me = lax.axis_index("cp")
    own = me // 2
    core = me % 2

    def vec(i):
        return vecs[i:i + 1, :]

    def weight_copy(i, src, dst):
        return pltpu.make_async_copy(src, dst, w_sem.at[i])

    weights = [(wqkv_h, wqkv), (wout_h, wout), (wpq_h, wpq), (wup_h, wup), (wdown_h, wdown), (wpkv_h, wpkv), (pwout_h, pwout), (pwup_h, pwup), (pwdown_h, pwdown)]

    def start_weight(i):
        weight_copy(i, *weights[i]).start()

    def wait_weight(i):
        weight_copy(i, *weights[i]).wait()

    def local_copy(j):
        return pltpu.make_async_copy(images.at[me * per + j], xbuf.at[j, me], recv_sem.at[j, me])

    deltas = [0]
    for d in range(1, nch // 2 + 1):
        deltas.append(d)
        if nch - d != d:
            deltas.append(nch - d)

    def remote(src, dst, send, recv, device):
        return pltpu.make_async_remote_copy(
            src_ref=src, dst_ref=dst, send_sem=send, recv_sem=recv, device_id={"cp": device}, device_id_type=pl.DeviceIdType.MESH)

    relayed = nch == 4

    def chip_core(delta, c):
        return ((own + delta + nch) % nch) * 2 + c

    def sends(j):
        copies = []

        def add(block, dst, recv, device):
            copies.append(remote(images.at[block * per + j], dst, send_sem.at[j, len(copies)], recv, device))

        for up in (0, 1) if relayed else ():
            add(chip_core(2, up), rel.at[j, up], rel_sem.at[j, up], chip_core(1 - 2 * up, core))
        for delta in deltas:
            for cc in (0, 1):
                if (delta == 0 and cc == 0) or (relayed and delta == 2):
                    continue
                dst = chip_core(delta, (core + cc) % 2)
                add(dst, xbuf.at[j, me], recv_sem.at[j, me], dst)
        return copies

    def forwards(j):
        copies = []
        for up in (0, 1) if relayed else ():
            source = chip_core(2 * up - 1, core)
            copies.append(remote(rel.at[j, up], xbuf.at[j, source], fwd_sem.at[j, up], recv_sem.at[j, source], chip_core(1 - 2 * up, up)))
        return copies

    def start_forwards(j):
        for up, copy in enumerate(forwards(j)):
            pltpu.make_async_copy(images.at[0], rel.at[j, up], rel_sem.at[j, up]).wait()
            copy.start()

    small_copies = [pltpu.make_async_copy(src, dst, v_sem.at[i]) for i, (src, dst) in enumerate(zip((*smalls, probe_h), (*small_bufs, probe)))]
    start_weight(0)
    for j in range(per):
        local_copy(j).start()
    for copy in small_copies:
        copy.start()

    barrier = pltpu.get_barrier_semaphore()
    for s in range(1, n):
        pl.semaphore_signal(barrier, inc=1, device_id={"cp": (me + s) % n}, device_id_type=pl.DeviceIdType.MESH)
    pl.semaphore_wait(barrier, n - 1)

    for copy in sends(0):
        copy.start()
    for i in range(1, len(weights)):
        start_weight(i)

    for copy in small_copies:
        copy.wait()
    for i, buf in enumerate(small_bufs[:12]):
        vecs[i:i + 1, :] = buf[...].reshape(1, width)
    bqkv_b, pbq_b, pbkv_b, bup_b, pbup_b = small_bufs[12:]
    for h in range(heads):
        lanes = slice(h * head_dim, (h + 1) * head_dim)
        for i, row in enumerate((B_Q, B_K, B_V)):
            vecs[row:row + 1, lanes] = bqkv_b[i, h:h + 1, :]
        vecs[P_BQ:P_BQ + 1, lanes] = pbq_b[h:h + 1, :]
        for i, row in enumerate((P_BK, P_BV)):
            vecs[row:row + 1, lanes] = pbkv_b[h, i:i + 1, :]
    for hc in range(hid_chunks):
        span = slice(hc * width, (hc + 1) * width)
        vecs[N_FIXED + hc:N_FIXED + hc + 1, :] = bup_b[span].reshape(1, width)
        vecs[N_FIXED + hid_chunks + hc:N_FIXED + hid_chunks + hc + 1, :] = pbup_b[span].reshape(1, width)
    for slot, row in enumerate((B_Q, B_V)):
        cols[slot] = jnp.transpose(jnp.broadcast_to(vec(row), (LANES, width)))
    qz[...] = jnp.zeros_like(qz)
    abuf[...] = jnp.zeros_like(abuf)
    wait_weight(0)

    def col_bias(slot, lo, size):
        tile = cols[slot, lo:lo + size, :]
        return jnp.concatenate([tile] * (BLOCK // LANES), axis=1)

    def wait_source(j, src):
        pltpu.make_async_copy(images.at[0], xbuf.at[j, src], recv_sem.at[j, src]).wait()

    s_refs = ((s00, s01), (s10, s11))
    p_refs = ((p00, p01), (p10, p11))

    def one_image(j, carry):
        def chip_of(k):
            return (own + deltas[k]) % nch

        def enter(k):
            x = xbuf[j, pl.ds(chip_of(k) * 2, 2)].reshape(BLOCK, width)
            for r0 in range(0, BLOCK, 64):
                hbuf[k % 2, r0:r0 + 64, :] = layer_norm(x[r0:r0 + 64].astype(F32), vec(LN1_G), vec(LN1_B)).astype(BF16)

        def project(k):
            tok = pl.multiple_of(chip_of(k) * BLOCK, BLOCK)
            h = hbuf[k % 2]
            for r, size, qt in halves_t(wqkv, 0, width, h):
                qt = (qt + col_bias(0, r, size)).astype(BF16)
                for h0 in range(0, size, head_dim):
                    hd = (r + h0) // head_dim
                    off = (hd % 2) * head_dim
                    qz[hd, off:off + head_dim, pl.ds(tok, BLOCK)] = qt[h0:h0 + head_dim]
            for r, size, v in halves_t(wqkv, 2 * width, width, h):
                vt[r:r + size, pl.ds(tok, BLOCK)] = (v + col_bias(1, r, size)).astype(BF16)
            kbuf[pl.ds(tok, BLOCK), :] = (dot_t(h, wqkv[width:2 * width, :]) + vec(B_K)).astype(BF16)

        def wait_chip(k):
            wait_source(j, chip_of(k) * 2)
            wait_source(j, chip_of(k) * 2 + 1)

        @pl.when(j == 0)
        def _():
            for k in range(nch):
                if k == 1:
                    start_forwards(0)
                    for later in range(1, per):
                        for copy in sends(later):
                            copy.start()
                wait_chip(k)
                enter(k)
                project(k)

        @pl.when(j > 0)
        def _():
            for k in range(nch):
                wait_chip(k)
            enter(0)
            for k in range(nch):
                if k + 1 < nch:
                    enter(k + 1)
                project(k)

        def qk(step, slot):
            hp, qb = step // nq, step % nq
            keys = kbuf[:, pl.ds(pl.multiple_of(hp * LANES, LANES), LANES)]
            for hh in (0, 1):
                q = qz[hp * 2 + hh, :, pl.ds(pl.multiple_of(qb * BLOCK, BLOCK), BLOCK)]
                s = dot(keys, q)
                s_refs[slot][hh][...] = s
                mbuf[slot, hh] = jnp.max(s.reshape(tokens // 8, 8, BLOCK), axis=0)

        def softmax_pv(step, slot):
            hp, qb = step // nq, step % nq
            outs = []
            for hh in (0, 1):
                s_ref, p_ref = s_refs[slot][hh], p_refs[slot][hh]
                m = jnp.max(mbuf[slot, hh], axis=0, keepdims=True)
                total = jnp.zeros((8, BLOCK), F32)
                for kc in range(0, tokens, LANES):
                    p = jnp.exp2((s_ref[kc:kc + LANES, :] - m) * exp_scale)
                    total = total + jnp.sum(p.reshape(LANES // 8, 8, BLOCK), axis=0)
                    p_ref[kc:kc + LANES, :] = p.astype(BF16)
                row_sum = jnp.sum(total, axis=0, keepdims=True)
                v = vt[pl.ds(pl.multiple_of(hp * LANES + hh * head_dim, head_dim), head_dim), :]
                outs.append(dot(v, p_ref[...]) * (1.0 / row_sum))
            pair = jnp.transpose(jnp.concatenate(outs, axis=0)).astype(BF16)
            ctx[pl.ds(pl.multiple_of(qb * BLOCK, BLOCK), BLOCK), pl.ds(pl.multiple_of(hp * LANES, LANES), LANES)] = pair

        qk(0, 0)

        def attend(i, c):
            for k in range(UNROLL):
                qk((UNROLL * i + k + 1) % nsteps, (k + 1) % 2)
                softmax_pv(UNROLL * i + k, k % 2)
            return c

        lax.fori_loop(0, nsteps // UNROLL, attend, 0)

        @pl.when(j == 0)
        def _():
            for later in range(1, per):
                start_forwards(later)
            for i in range(1, 6):
                wait_weight(i)
            q16 = jnp.broadcast_to(probe[...], (16, width))
            u = dot_t(q16, wpq[...]) + vec(P_BQ)
            row = lax.broadcasted_iota(jnp.int32, (16, width), 0)
            col = lax.broadcasted_iota(jnp.int32, (16, width), 1)
            ubuf[...] = jnp.where(col // head_dim == row, u, 0.0).astype(BF16)

        def pool(t, block):
            start = pl.multiple_of((block % nq) * BLOCK, BLOCK)
            kv = dot_t(zbuf[t], wpkv[...])
            score[:, pl.ds(start, BLOCK)] = dot_t(ubuf[...], (kv[:, 0:width] + vec(P_BK)).astype(BF16))
            pvbuf[pl.ds(start, BLOCK), :] = (kv[:, width:2 * width] + vec(P_BV)).astype(BF16)

        def tail(i, c):
            starts = [pl.multiple_of((2 * i + t) * BLOCK, BLOCK) for t in (0, 1)]

            def resid(t):
                chip = 2 * i + t
                x = xbuf[j, pl.ds(chip * 2, 2)].reshape(BLOCK, width)
                a = dot(ctx[pl.ds(starts[t], BLOCK), :], wout[...])
                rbuf[t] = (x.astype(F32) + a + vec(B_OUT)).astype(BF16)

            def norm(t):
                for r0 in range(0, BLOCK, 64):
                    nbuf[t, r0:r0 + 64, :] = layer_norm(rbuf[t, r0:r0 + 64, :].astype(F32), vec(LN2_G), vec(LN2_B)).astype(BF16)

            def up(t):
                for hc in range(hid_chunks):
                    cols_ = slice(hc * width, (hc + 1) * width)
                    hid[t, :, cols_] = gelu(dot(nbuf[t], wup[:, cols_]) + vec(N_FIXED + hc)).astype(BF16)

            def down(t, row_parts):
                for lo, size, parts in row_parts:
                    rows = slice(lo, lo + size)
                    y = jnp.concatenate([dot(hid[t, rows, :], wdown[:, c0:c1]) for c0, c1 in parts], axis=1)
                    y = (rbuf[t, rows, :].astype(F32) + y + vec(B_DOWN)).astype(BF16)
                    for r0 in range(0, size, 64):
                        zbuf[t, lo + r0:lo + r0 + 64, :] = layer_norm(y[r0:r0 + 64].astype(F32), vec(LNF_G), vec(LNF_B)).astype(BF16)

            whole = [(0, width)]
            row_halves = [(0, BLOCK // 2, whole), (BLOCK // 2, BLOCK // 2, whole)]

            resid(0)
            resid(1)
            pool(1, 2 * i + nq - 1)
            norm(0)
            up(0)
            norm(1)
            up(1)
            down(0, [(0, BLOCK, whole)])
            down(1, row_halves)
            pool(0, 2 * i)
            return c

        zbuf[1] = jnp.zeros((BLOCK, width), BF16)
        lax.fori_loop(0, nq // 2, tail, 0)
        pool(1, nq - 1)

        s = score[...]
        w = jnp.exp2((s - jnp.max(s, axis=-1, keepdims=True)) * exp_scale)
        a = dot(w.astype(BF16), pvbuf[...]) / jnp.sum(w, axis=-1, keepdims=True)
        row = lax.broadcasted_iota(jnp.int32, (16, width), 0)
        col = lax.broadcasted_iota(jnp.int32, (16, width), 1)
        abuf[pl.ds(j, 1), :] = jnp.sum(jnp.where(col // head_dim == row, a, 0.0), axis=0, keepdims=True)
        return carry

    lax.fori_loop(0, per, one_image, 0)

    for i in range(6, len(weights)):
        wait_weight(i)
    o = (dot(abuf[...].astype(BF16), pwout[...]) + vec(P_BOUT)).astype(BF16).astype(F32)
    normed = layer_norm(o, vec(P_LN_G), vec(P_LN_B)).astype(BF16)
    emb = o + vec(P_BDOWN)
    for hc in range(hid_chunks):
        cols_ = slice(hc * width, (hc + 1) * width)
        m = gelu(dot(normed, pwup[:, cols_]) + vec(N_FIXED + hid_chunks + hc)).astype(BF16)
        emb = emb + dot(m, pwdown[cols_, :])
    gath[pl.ds(me, 1)] = emb[0:8][None]

    copies = []
    for s in range(1, n):
        copies.append(pltpu.make_async_remote_copy(
            src_ref=gath.at[me],
            dst_ref=gath.at[me],
            send_sem=gsend_sem.at[s],
            recv_sem=grecv_sem.at[me],
            device_id={"cp": (me + s) % n},
            device_id_type=pl.DeviceIdType.MESH,
        ))
    for copy in copies:
        copy.start()
    for j in range(per):
        for copy in sends(j) + forwards(j):
            copy.wait_send()
    for s in range(1, n):
        src = (me + s) % n
        pltpu.make_async_remote_copy(
            src_ref=gath.at[src], dst_ref=gath.at[src], send_sem=gsend_sem.at[s], recv_sem=grecv_sem.at[src],
            device_id={"cp": src}, device_id_type=pl.DeviceIdType.MESH,
        ).wait_recv()
    for copy in copies:
        copy.wait_send()
    for s in range(n):
        out_ref[s * per:(s + 1) * per, :] = gath[s, 0:per, :]


def solution(mesh):
    n = mesh.shape["cp"]

    def device_step(images, ln1_scale, ln1_bias, w_qkv, b_qkv, w_out, b_out, ln2_scale, ln2_bias, w_up, b_up, w_down, b_down, lnf_scale, lnf_bias, pool_probe, pool_wq, pool_bq, pool_wkv, pool_bkv, pool_wout, pool_bout, pool_ln_scale, pool_ln_bias, pool_w_up, pool_b_up, pool_w_down, pool_b_down):
        count, run, width = images.shape
        heads, head_dim = w_qkv.shape[2:]
        mlp = w_up.shape[1]
        per = count // n
        tokens = n * run
        wqkv_t = jnp.transpose(w_qkv, (1, 2, 3, 0)).reshape(3 * width, width)
        wpkv_t = jnp.transpose(pool_wkv, (1, 2, 3, 0)).reshape(2 * width, width)
        wpq_t = jnp.transpose(pool_wq, (1, 2, 0)).reshape(width, width)
        wout2 = w_out.reshape(width, width)
        pwout2 = pool_wout.reshape(width, width)
        smalls = (ln1_scale, ln1_bias, b_out, ln2_scale, ln2_bias, b_down, lnf_scale, lnf_bias, pool_bout, pool_ln_scale, pool_ln_bias, pool_b_down, b_qkv, pool_bq, jnp.transpose(pool_bkv, (1, 0, 2)), b_up, pool_b_up)
        any_spec = pl.BlockSpec(memory_space=pl.ANY)
        vmem_spec = pl.BlockSpec(memory_space=pltpu.VMEM)
        big = (images, wqkv_t, wout2, w_up, w_down, wpkv_t, wpq_t, pwout2, pool_w_up, pool_w_down)
        scratch = [pltpu.VMEM(w.shape, BF16) for w in big[1:]] + [
            pltpu.VMEM((per, n, run, width), BF16),
            pltpu.VMEM((heads, LANES, tokens), BF16),
            pltpu.VMEM((tokens, width), BF16),
            pltpu.VMEM((width, tokens), BF16),
            *[pltpu.VMEM((tokens, BLOCK), F32) for _ in range(4)],
            *[pltpu.VMEM((tokens, BLOCK), BF16) for _ in range(4)],
            pltpu.VMEM((2, 2, 8, BLOCK), F32),
            pltpu.VMEM((tokens, width), BF16),
            pltpu.VMEM((2, BLOCK, width), BF16),
            pltpu.VMEM((2, BLOCK, width), BF16),
            pltpu.VMEM((2, BLOCK, width), BF16),
            pltpu.VMEM((2, BLOCK, mlp), BF16),
            pltpu.VMEM((2, BLOCK, width), BF16),
            pltpu.VMEM((16, tokens), F32),
            pltpu.VMEM((tokens, width), BF16),
            pltpu.VMEM((16, width), BF16),
            pltpu.VMEM((2, width, LANES), F32),
            pltpu.VMEM((16, width), F32),
            pltpu.VMEM((n, 8, width), F32),
            pltpu.VMEM((per, 2, run, width), BF16),
            pltpu.VMEM((N_FIXED + 2 * mlp // width, width), F32),
            pltpu.VMEM(pool_probe.shape, BF16),
            *[pltpu.VMEM(v.shape, F32) for v in smalls],
            pltpu.SemaphoreType.DMA((per, n)),
            pltpu.SemaphoreType.DMA((per, n)),
            pltpu.SemaphoreType.DMA((per, 2)),
            pltpu.SemaphoreType.DMA((per, 2)),
            pltpu.SemaphoreType.DMA((len(big) - 1,)),
            pltpu.SemaphoreType.DMA((n,)),
            pltpu.SemaphoreType.DMA((n,)),
            pltpu.SemaphoreType.DMA((N_SMALL + 1,)),
        ]
        return pl.pallas_call(
            functools.partial(kernel, (n, per, heads, head_dim, width, mlp)),
            out_shape=jax.ShapeDtypeStruct((count, width), F32),
            in_specs=[any_spec] * (len(big) + len(smalls) + 1),
            out_specs=vmem_spec,
            scratch_shapes=scratch,
            compiler_params=pltpu.CompilerParams(collective_id=0, has_side_effects=True, vmem_limit_bytes=67043328),
            name="encoder_pool",
        )(*big, *smalls, pool_probe)

    in_specs = (P("dp", "cp", None),) + (P(),) * 27
    return jax.shard_map(device_step, mesh=mesh, in_specs=in_specs, out_specs=P("dp", None), check_vma=False)
```

```python
import functools
import math

import jax
import jax.numpy as jnp
from jax import lax
from jax.experimental import pallas as pl
from jax.experimental.pallas import tpu as pltpu
from jax.sharding import PartitionSpec as P

EPSILON = 1e-6
LANES = 128
BLOCK = 256
UNROLL = 8
F32 = jnp.float32
BF16 = jnp.bfloat16

(LN1_G, LN1_B, B_OUT, LN2_G, LN2_B, B_DOWN, LNF_G, LNF_B, P_BOUT, P_LN_G, P_LN_B, P_BDOWN, B_Q, B_K, B_V, P_BQ, P_BK, P_BV) = range(18)
N_FIXED = 18
N_SMALL = 17


def layer_norm(values, ln_gain, ln_shift):
    row_mean = jnp.mean(values, axis=-1, keepdims=True)
    centered = values - row_mean
    variance = jnp.mean(centered * centered, axis=-1, keepdims=True)
    return centered * lax.rsqrt(variance + EPSILON) * ln_gain + ln_shift


def gelu(x):
    return jax.nn.gelu(x, approximate=True)


def dot(a, b):
    return lax.dot_general(a, b, (((1,), (0,)), ((), ())), preferred_element_type=F32)


def dot_t(a, b):
    return lax.dot_general(a, b, (((1,), (1,)), ((), ())), preferred_element_type=F32)


def halves_t(a_ref, lo, size, b):
    half = size // 2
    return [(r, half, dot_t(a_ref[lo + r:lo + r + half, :], b)) for r in (0, half)]


def kernel(cfg, images, wqkv_h, wout_h, wup_h, wdown_h, wpkv_h, wpq_h, pwout_h, pwup_h, pwdown_h, *rest):
    n, per, heads, head_dim, width, mlp = cfg
    smalls = rest[:N_SMALL]
    (probe_h, out_ref,
           wqkv, wout, wup, wdown, wpkv, wpq, pwout, pwup, pwdown,
           xbuf, qz, kbuf, vt, s00, s01, s10, s11, p00, p01, p10, p11, mbuf, ctx, hbuf, rbuf, nbuf, hid, zbuf,
           score, pvbuf, ubuf, cols, abuf, gath, rel, vecs, probe, *tail_refs) = rest[N_SMALL:]
    small_bufs = tail_refs[:N_SMALL]
    send_sem, recv_sem, rel_sem, fwd_sem, w_sem, gsend_sem, grecv_sem, v_sem = tail_refs[N_SMALL:]
    run = images.shape[1]
    tokens = n * run
    nch = n // 2
    hid_chunks = mlp // width
    pairs = heads // 2
    nq = tokens // BLOCK
    nsteps = pairs * nq
    exp_scale = math.log2(math.e) * head_dim ** -0.5
    me = lax.axis_index("cp")
    own = me // 2
    core = me % 2

    def vec(i):
        return vecs[i:i + 1, :]

    def weight_copy(i, src, dst):
        return pltpu.make_async_copy(src, dst, w_sem.at[i])

    weights = [(wqkv_h, wqkv), (wout_h, wout), (wpq_h, wpq), (wup_h, wup), (wdown_h, wdown), (wpkv_h, wpkv), (pwout_h, pwout), (pwup_h, pwup), (pwdown_h, pwdown)]

    def start_weight(i):
        weight_copy(i, *weights[i]).start()

    def wait_weight(i):
        weight_copy(i, *weights[i]).wait()

    def local_copy(j):
        return pltpu.make_async_copy(images.at[me * per + j], xbuf.at[j, me], recv_sem.at[j, me])

    deltas = [0]
    for d in range(1, nch // 2 + 1):
        deltas.append(d)
        if nch - d != d:
            deltas.append(nch - d)

    def remote(src, dst, send, recv, device):
        return pltpu.make_async_remote_copy(
            src_ref=src, dst_ref=dst, send_sem=send, recv_sem=recv, device_id={"cp": device}, device_id_type=pl.DeviceIdType.MESH)

    relayed = nch == 4

    def chip_core(delta, c):
        return ((own + delta + nch) % nch) * 2 + c

    def sends(j):
        copies = []

        def add(block, dst, recv, device):
            copies.append(remote(images.at[block * per + j], dst, send_sem.at[j, len(copies)], recv, device))

        for up in (0, 1) if relayed else ():
            add(chip_core(2, up), rel.at[j, up], rel_sem.at[j, up], chip_core(1 - 2 * up, core))
        for delta in deltas:
            for cc in (0, 1):
                if (delta == 0 and cc == 0) or (relayed and delta == 2):
                    continue
                dst = chip_core(delta, (core + cc) % 2)
                add(dst, xbuf.at[j, me], recv_sem.at[j, me], dst)
        return copies

    def forwards(j):
        copies = []
        for up in (0, 1) if relayed else ():
            source = chip_core(2 * up - 1, core)
            copies.append(remote(rel.at[j, up], xbuf.at[j, source], fwd_sem.at[j, up], recv_sem.at[j, source], chip_core(1 - 2 * up, up)))
        return copies

    def start_forwards(j):
        for up, copy in enumerate(forwards(j)):
            pltpu.make_async_copy(images.at[0], rel.at[j, up], rel_sem.at[j, up]).wait()
            copy.start()

    small_copies = [pltpu.make_async_copy(src, dst, v_sem.at[i]) for i, (src, dst) in enumerate(zip((*smalls, probe_h), (*small_bufs, probe)))]
    start_weight(0)
    for j in range(per):
        local_copy(j).start()
    for copy in small_copies:
        copy.start()

    barrier = pltpu.get_barrier_semaphore()
    for s in range(1, n):
        pl.semaphore_signal(barrier, inc=1, device_id={"cp": (me + s) % n}, device_id_type=pl.DeviceIdType.MESH)
    pl.semaphore_wait(barrier, n - 1)

    for copy in sends(0):
        copy.start()
    for i in (2, 1, *range(3, len(weights))):
        start_weight(i)

    for copy in small_copies:
        copy.wait()
    for i, buf in enumerate(small_bufs[:12]):
        vecs[i:i + 1, :] = buf[...].reshape(1, width)
    bqkv_b, pbq_b, pbkv_b, bup_b, pbup_b = small_bufs[12:]
    for h in range(heads):
        lanes = slice(h * head_dim, (h + 1) * head_dim)
        for i, row in enumerate((B_Q, B_K, B_V)):
            vecs[row:row + 1, lanes] = bqkv_b[i, h:h + 1, :]
        vecs[P_BQ:P_BQ + 1, lanes] = pbq_b[h:h + 1, :]
        for i, row in enumerate((P_BK, P_BV)):
            vecs[row:row + 1, lanes] = pbkv_b[h, i:i + 1, :]
    for hc in range(hid_chunks):
        span = slice(hc * width, (hc + 1) * width)
        vecs[N_FIXED + hc:N_FIXED + hc + 1, :] = bup_b[span].reshape(1, width)
        vecs[N_FIXED + hid_chunks + hc:N_FIXED + hid_chunks + hc + 1, :] = pbup_b[span].reshape(1, width)
    for slot, row in enumerate((B_Q, B_V)):
        cols[slot] = jnp.transpose(jnp.broadcast_to(vec(row), (LANES, width)))
    qz[...] = jnp.zeros_like(qz)
    abuf[...] = jnp.zeros_like(abuf)
    zbuf[1] = jnp.zeros((BLOCK, width), BF16)
    wait_weight(0)

    def col_bias(slot, lo, size):
        tile = cols[slot, lo:lo + size, :]
        return jnp.concatenate([tile] * (BLOCK // LANES), axis=1)

    def wait_source(j, src):
        pltpu.make_async_copy(images.at[0], xbuf.at[j, src], recv_sem.at[j, src]).wait()

    s_refs = ((s00, s01), (s10, s11))
    p_refs = ((p00, p01), (p10, p11))

    def pool(t, block):
        start = pl.multiple_of((block % nq) * BLOCK, BLOCK)
        kv = dot_t(zbuf[t], wpkv[...])
        score[:, pl.ds(start, BLOCK)] = dot_t(ubuf[...], (kv[:, 0:width] + vec(P_BK)).astype(BF16))
        pvbuf[pl.ds(start, BLOCK), :] = (kv[:, width:2 * width] + vec(P_BV)).astype(BF16)

    def pool_query():
        q16 = jnp.broadcast_to(probe[...], (16, width))
        u = dot_t(q16, wpq[...]) + vec(P_BQ)
        row = lax.broadcasted_iota(jnp.int32, (16, width), 0)
        col = lax.broadcasted_iota(jnp.int32, (16, width), 1)
        ubuf[...] = jnp.where(col // head_dim == row, u, 0.0).astype(BF16)

    def finish_pool(image):
        pool(1, nq - 1)
        s = score[...]
        w = jnp.exp2((s - jnp.max(s, axis=-1, keepdims=True)) * exp_scale)
        a = dot(w.astype(BF16), pvbuf[...]) / jnp.sum(w, axis=-1, keepdims=True)
        row = lax.broadcasted_iota(jnp.int32, (16, width), 0)
        col = lax.broadcasted_iota(jnp.int32, (16, width), 1)
        abuf[pl.ds(image, 1), :] = jnp.sum(jnp.where(col // head_dim == row, a, 0.0), axis=0, keepdims=True)

    def one_image(j, carry):
        def chip_of(k):
            return (own + deltas[k]) % nch

        def enter(k):
            x = xbuf[j, pl.ds(chip_of(k) * 2, 2)].reshape(BLOCK, width)
            for r0 in range(0, BLOCK, 64):
                hbuf[k % 2, r0:r0 + 64, :] = layer_norm(x[r0:r0 + 64].astype(F32), vec(LN1_G), vec(LN1_B)).astype(BF16)

        def project(k):
            tok = pl.multiple_of(chip_of(k) * BLOCK, BLOCK)
            h = hbuf[k % 2]
            for r, size, qt in halves_t(wqkv, 0, width, h):
                qt = (qt + col_bias(0, r, size)).astype(BF16)
                for h0 in range(0, size, head_dim):
                    hd = (r + h0) // head_dim
                    off = (hd % 2) * head_dim
                    qz[hd, off:off + head_dim, pl.ds(tok, BLOCK)] = qt[h0:h0 + head_dim]
            for r, size, v in halves_t(wqkv, 2 * width, width, h):
                vt[r:r + size, pl.ds(tok, BLOCK)] = (v + col_bias(1, r, size)).astype(BF16)
            kbuf[pl.ds(tok, BLOCK), :] = (dot_t(h, wqkv[width:2 * width, :]) + vec(B_K)).astype(BF16)

        def wait_chip(k):
            wait_source(j, chip_of(k) * 2)
            wait_source(j, chip_of(k) * 2 + 1)

        @pl.when(j == 0)
        def _():
            for k in range(nch):
                if k == 1:
                    start_forwards(0)
                    for later in range(1, per):
                        for copy in sends(later):
                            copy.start()
                    wait_weight(2)
                    pool_query()
                wait_chip(k)
                enter(k)
                project(k)

        @pl.when(j > 0)
        def _():
            for k in range(nch):
                wait_chip(k)
            finish_pool(j - 1)
            enter(0)
            for k in range(nch):
                if k + 1 < nch:
                    enter(k + 1)
                project(k)

        def qk(step, slot):
            hp, qb = step // nq, step % nq
            keys = kbuf[:, pl.ds(pl.multiple_of(hp * LANES, LANES), LANES)]
            for hh in (0, 1):
                q = qz[hp * 2 + hh, :, pl.ds(pl.multiple_of(qb * BLOCK, BLOCK), BLOCK)]
                s = dot(keys, q)
                s_refs[slot][hh][...] = s
                mbuf[slot, hh] = jnp.max(s.reshape(tokens // 8, 8, BLOCK), axis=0)

        def softmax_pv(step, slot):
            hp, qb = step // nq, step % nq
            outs = []
            for hh in (0, 1):
                s_ref, p_ref = s_refs[slot][hh], p_refs[slot][hh]
                m = jnp.max(mbuf[slot, hh], axis=0, keepdims=True)
                total = jnp.zeros((8, BLOCK), F32)
                for kc in range(0, tokens, LANES):
                    p = jnp.exp2((s_ref[kc:kc + LANES, :] - m) * exp_scale)
                    total = total + jnp.sum(p.reshape(LANES // 8, 8, BLOCK), axis=0)
                    p_ref[kc:kc + LANES, :] = p.astype(BF16)
                row_sum = jnp.sum(total, axis=0, keepdims=True)
                v = vt[pl.ds(pl.multiple_of(hp * LANES + hh * head_dim, head_dim), head_dim), :]
                outs.append(dot(v, p_ref[...]) * (1.0 / row_sum))
            pair = jnp.transpose(jnp.concatenate(outs, axis=0)).astype(BF16)
            ctx[pl.ds(pl.multiple_of(qb * BLOCK, BLOCK), BLOCK), pl.ds(pl.multiple_of(hp * LANES, LANES), LANES)] = pair

        qk(0, 0)

        def attend(i, c):
            for k in range(UNROLL):
                qk((UNROLL * i + k + 1) % nsteps, (k + 1) % 2)
                softmax_pv(UNROLL * i + k, k % 2)
            return c

        lax.fori_loop(0, nsteps // UNROLL, attend, 0)

        @pl.when(j == 0)
        def _():
            for later in range(1, per):
                start_forwards(later)
            for i in (1, 3, 4, 5):
                wait_weight(i)

        def tail(i, c):
            starts = [pl.multiple_of((2 * i + t) * BLOCK, BLOCK) for t in (0, 1)]

            def resid(t):
                chip = 2 * i + t
                x = xbuf[j, pl.ds(chip * 2, 2)].reshape(BLOCK, width)
                a = dot(ctx[pl.ds(starts[t], BLOCK), :], wout[...])
                rbuf[t] = (x.astype(F32) + a + vec(B_OUT)).astype(BF16)

            def norm(t):
                for r0 in range(0, BLOCK, 64):
                    nbuf[t, r0:r0 + 64, :] = layer_norm(rbuf[t, r0:r0 + 64, :].astype(F32), vec(LN2_G), vec(LN2_B)).astype(BF16)

            def up(t):
                for hc in range(hid_chunks):
                    cols_ = slice(hc * width, (hc + 1) * width)
                    hid[t, :, cols_] = gelu(dot(nbuf[t], wup[:, cols_]) + vec(N_FIXED + hc)).astype(BF16)

            def down(t, row_parts):
                for lo, size, parts in row_parts:
                    rows = slice(lo, lo + size)
                    y = jnp.concatenate([dot(hid[t, rows, :], wdown[:, c0:c1]) for c0, c1 in parts], axis=1)
                    y = (rbuf[t, rows, :].astype(F32) + y + vec(B_DOWN)).astype(BF16)
                    for r0 in range(0, size, 64):
                        zbuf[t, lo + r0:lo + r0 + 64, :] = layer_norm(y[r0:r0 + 64].astype(F32), vec(LNF_G), vec(LNF_B)).astype(BF16)

            whole = [(0, width)]
            row_halves = [(0, BLOCK // 2, whole), (BLOCK // 2, BLOCK // 2, whole)]

            resid(0)
            resid(1)
            pool(1, 2 * i + nq - 1)
            norm(0)
            up(0)
            norm(1)
            up(1)
            down(0, [(0, BLOCK, whole)])
            down(1, row_halves)
            pool(0, 2 * i)
            return c

        lax.fori_loop(0, nq // 2, tail, 0)
        return carry

    lax.fori_loop(0, per, one_image, 0)
    finish_pool(per - 1)

    for i in range(6, len(weights)):
        wait_weight(i)
    o = (dot(abuf[...].astype(BF16), pwout[...]) + vec(P_BOUT)).astype(BF16).astype(F32)
    normed = layer_norm(o, vec(P_LN_G), vec(P_LN_B)).astype(BF16)
    emb = o + vec(P_BDOWN)
    for hc in range(hid_chunks):
        cols_ = slice(hc * width, (hc + 1) * width)
        m = gelu(dot(normed, pwup[:, cols_]) + vec(N_FIXED + hid_chunks + hc)).astype(BF16)
        emb = emb + dot(m, pwdown[cols_, :])
    gath[pl.ds(me, 1)] = emb[0:8][None]

    copies = []
    for s in range(1, n):
        copies.append(pltpu.make_async_remote_copy(
            src_ref=gath.at[me],
            dst_ref=gath.at[me],
            send_sem=gsend_sem.at[s],
            recv_sem=grecv_sem.at[me],
            device_id={"cp": (me + s) % n},
            device_id_type=pl.DeviceIdType.MESH,
        ))
    for copy in copies:
        copy.start()
    for j in range(per):
        for copy in sends(j) + forwards(j):
            copy.wait_send()
    for s in range(1, n):
        src = (me + s) % n
        pltpu.make_async_remote_copy(
            src_ref=gath.at[src], dst_ref=gath.at[src], send_sem=gsend_sem.at[s], recv_sem=grecv_sem.at[src],
            device_id={"cp": src}, device_id_type=pl.DeviceIdType.MESH,
        ).wait_recv()
    for copy in copies:
        copy.wait_send()
    for s in range(n):
        out_ref[s * per:(s + 1) * per, :] = gath[s, 0:per, :]


def solution(mesh):
    n = mesh.shape["cp"]

    def device_step(images, ln1_scale, ln1_bias, w_qkv, b_qkv, w_out, b_out, ln2_scale, ln2_bias, w_up, b_up, w_down, b_down, lnf_scale, lnf_bias, pool_probe, pool_wq, pool_bq, pool_wkv, pool_bkv, pool_wout, pool_bout, pool_ln_scale, pool_ln_bias, pool_w_up, pool_b_up, pool_w_down, pool_b_down):
        count, run, width = images.shape
        heads, head_dim = w_qkv.shape[2:]
        mlp = w_up.shape[1]
        per = count // n
        tokens = n * run
        wqkv_t = jnp.transpose(w_qkv, (1, 2, 3, 0)).reshape(3 * width, width)
        wpkv_t = jnp.transpose(pool_wkv, (1, 2, 3, 0)).reshape(2 * width, width)
        wpq_t = jnp.transpose(pool_wq, (1, 2, 0)).reshape(width, width)
        wout2 = w_out.reshape(width, width)
        pwout2 = pool_wout.reshape(width, width)
        smalls = (ln1_scale, ln1_bias, b_out, ln2_scale, ln2_bias, b_down, lnf_scale, lnf_bias, pool_bout, pool_ln_scale, pool_ln_bias, pool_b_down, b_qkv, pool_bq, jnp.transpose(pool_bkv, (1, 0, 2)), b_up, pool_b_up)
        any_spec = pl.BlockSpec(memory_space=pl.ANY)
        vmem_spec = pl.BlockSpec(memory_space=pltpu.VMEM)
        big = (images, wqkv_t, wout2, w_up, w_down, wpkv_t, wpq_t, pwout2, pool_w_up, pool_w_down)
        scratch = [pltpu.VMEM(w.shape, BF16) for w in big[1:]] + [
            pltpu.VMEM((per, n, run, width), BF16),
            pltpu.VMEM((heads, LANES, tokens), BF16),
            pltpu.VMEM((tokens, width), BF16),
            pltpu.VMEM((width, tokens), BF16),
            *[pltpu.VMEM((tokens, BLOCK), F32) for _ in range(4)],
            *[pltpu.VMEM((tokens, BLOCK), BF16) for _ in range(4)],
            pltpu.VMEM((2, 2, 8, BLOCK), F32),
            pltpu.VMEM((tokens, width), BF16),
            pltpu.VMEM((2, BLOCK, width), BF16),
            pltpu.VMEM((2, BLOCK, width), BF16),
            pltpu.VMEM((2, BLOCK, width), BF16),
            pltpu.VMEM((2, BLOCK, mlp), BF16),
            pltpu.VMEM((2, BLOCK, width), BF16),
            pltpu.VMEM((16, tokens), F32),
            pltpu.VMEM((tokens, width), BF16),
            pltpu.VMEM((16, width), BF16),
            pltpu.VMEM((2, width, LANES), F32),
            pltpu.VMEM((16, width), F32),
            pltpu.VMEM((n, 8, width), F32),
            pltpu.VMEM((per, 2, run, width), BF16),
            pltpu.VMEM((N_FIXED + 2 * mlp // width, width), F32),
            pltpu.VMEM(pool_probe.shape, BF16),
            *[pltpu.VMEM(v.shape, F32) for v in smalls],
            pltpu.SemaphoreType.DMA((per, n)),
            pltpu.SemaphoreType.DMA((per, n)),
            pltpu.SemaphoreType.DMA((per, 2)),
            pltpu.SemaphoreType.DMA((per, 2)),
            pltpu.SemaphoreType.DMA((len(big) - 1,)),
            pltpu.SemaphoreType.DMA((n,)),
            pltpu.SemaphoreType.DMA((n,)),
            pltpu.SemaphoreType.DMA((N_SMALL + 1,)),
        ]
        return pl.pallas_call(
            functools.partial(kernel, (n, per, heads, head_dim, width, mlp)),
            out_shape=jax.ShapeDtypeStruct((count, width), F32),
            in_specs=[any_spec] * (len(big) + len(smalls) + 1),
            out_specs=vmem_spec,
            scratch_shapes=scratch,
            compiler_params=pltpu.CompilerParams(collective_id=0, has_side_effects=True, vmem_limit_bytes=67043328),
            name="encoder_pool",
        )(*big, *smalls, pool_probe)

    in_specs = (P("dp", "cp", None),) + (P(),) * 27
    return jax.shard_map(device_step, mesh=mesh, in_specs=in_specs, out_specs=P("dp", None), check_vma=False)
```

```python
import functools
import math

import jax
import jax.numpy as jnp
from jax import lax
from jax.experimental import pallas as pl
from jax.experimental.pallas import tpu as pltpu
from jax.sharding import PartitionSpec as P

EPSILON = 1e-6
LANES = 128
BLOCK = 256
UNROLL = 8
F32 = jnp.float32
BF16 = jnp.bfloat16

(LN1_G, LN1_B, B_OUT, LN2_G, LN2_B, B_DOWN, LNF_G, LNF_B, P_BOUT, P_LN_G, P_LN_B, P_BDOWN, B_Q, B_K, B_V, P_BQ, P_BK, P_BV) = range(18)
N_FIXED = 18
N_SMALL = 17


def layer_norm(values, ln_gain, ln_shift):
    row_mean = jnp.mean(values, axis=-1, keepdims=True)
    centered = values - row_mean
    variance = jnp.mean(centered * centered, axis=-1, keepdims=True)
    return centered * lax.rsqrt(variance + EPSILON) * ln_gain + ln_shift


def gelu(x):
    return jax.nn.gelu(x, approximate=True)


def dot(a, b):
    return lax.dot_general(a, b, (((1,), (0,)), ((), ())), preferred_element_type=F32)


def dot_t(a, b):
    return lax.dot_general(a, b, (((1,), (1,)), ((), ())), preferred_element_type=F32)


def halves_t(a_ref, lo, size, b):
    half = size // 2
    return [(r, half, dot_t(a_ref[lo + r:lo + r + half, :], b)) for r in (0, half)]


def kernel(cfg, images, wqkv_h, wout_h, wup_h, wdown_h, wpkv_h, wpq_h, pwout_h, pwup_h, pwdown_h, *rest):
    n, per, heads, head_dim, width, mlp = cfg
    smalls = rest[:N_SMALL]
    (probe_h, out_ref,
           wqkv, wout, wup, wdown, wpkv, wpq, pwout, pwup, pwdown,
           xbuf, qz, kbuf, vt, s00, s01, s10, s11, p00, p01, p10, p11, mbuf, ctx, hbuf, rbuf, nbuf, hid, zbuf,
           score, pvbuf, ubuf, cols, abuf, gath, rel, vecs, probe, *tail_refs) = rest[N_SMALL:]
    small_bufs = tail_refs[:N_SMALL]
    send_sem, recv_sem, rel_sem, fwd_sem, w_sem, gsend_sem, grecv_sem, v_sem = tail_refs[N_SMALL:]
    run = images.shape[1]
    tokens = n * run
    nch = n // 2
    hid_chunks = mlp // width
    pairs = heads // 2
    nq = tokens // BLOCK
    nsteps = pairs * nq
    exp_scale = math.log2(math.e) * head_dim ** -0.5
    me = lax.axis_index("cp")
    own = me // 2
    core = me % 2

    def vec(i):
        return vecs[i:i + 1, :]

    def weight_copy(i, src, dst):
        return pltpu.make_async_copy(src, dst, w_sem.at[i])

    weights = [(wqkv_h, wqkv), (wout_h, wout), (wpq_h, wpq), (wup_h, wup), (wdown_h, wdown), (wpkv_h, wpkv), (pwout_h, pwout), (pwup_h, pwup), (pwdown_h, pwdown)]

    def start_weight(i):
        weight_copy(i, *weights[i]).start()

    def wait_weight(i):
        weight_copy(i, *weights[i]).wait()

    def local_copy(j):
        return pltpu.make_async_copy(images.at[me * per + j], xbuf.at[j, me], recv_sem.at[j, me])

    deltas = [0]
    for d in range(1, nch // 2 + 1):
        deltas.append(d)
        if nch - d != d:
            deltas.append(nch - d)

    def remote(src, dst, send, recv, device):
        return pltpu.make_async_remote_copy(
            src_ref=src, dst_ref=dst, send_sem=send, recv_sem=recv, device_id={"cp": device}, device_id_type=pl.DeviceIdType.MESH)

    relayed = nch == 4

    def chip_core(delta, c):
        return ((own + delta + nch) % nch) * 2 + c

    def sends(j):
        copies = []

        def add(block, dst, recv, device):
            copies.append(remote(images.at[block * per + j], dst, send_sem.at[j, len(copies)], recv, device))

        for up in (0, 1) if relayed else ():
            add(chip_core(2, up), rel.at[j, up], rel_sem.at[j, up], chip_core(1 - 2 * up, core))
        for delta in deltas:
            for cc in (0, 1):
                if (delta == 0 and cc == 0) or (relayed and delta == 2):
                    continue
                dst = chip_core(delta, (core + cc) % 2)
                add(dst, xbuf.at[j, me], recv_sem.at[j, me], dst)
        return copies

    def forwards(j):
        copies = []
        for up in (0, 1) if relayed else ():
            source = chip_core(2 * up - 1, core)
            copies.append(remote(rel.at[j, up], xbuf.at[j, source], fwd_sem.at[j, up], recv_sem.at[j, source], chip_core(1 - 2 * up, up)))
        return copies

    def start_forwards(j):
        for up, copy in enumerate(forwards(j)):
            pltpu.make_async_copy(images.at[0], rel.at[j, up], rel_sem.at[j, up]).wait()
            copy.start()

    small_copies = [pltpu.make_async_copy(src, dst, v_sem.at[i]) for i, (src, dst) in enumerate(zip((*smalls, probe_h), (*small_bufs, probe)))]
    start_weight(0)
    for j in range(per):
        local_copy(j).start()
    for copy in small_copies:
        copy.start()

    barrier = pltpu.get_barrier_semaphore()
    for s in range(1, n):
        pl.semaphore_signal(barrier, inc=1, device_id={"cp": (me + s) % n}, device_id_type=pl.DeviceIdType.MESH)
    pl.semaphore_wait(barrier, n - 1)

    for copy in sends(0):
        copy.start()
    start_weight(2)

    for copy in small_copies:
        copy.wait()
    for i, buf in enumerate(small_bufs[:12]):
        vecs[i:i + 1, :] = buf[...].reshape(1, width)
    bqkv_b, pbq_b, pbkv_b, bup_b, pbup_b = small_bufs[12:]
    for h in range(heads):
        lanes = slice(h * head_dim, (h + 1) * head_dim)
        for i, row in enumerate((B_Q, B_K, B_V)):
            vecs[row:row + 1, lanes] = bqkv_b[i, h:h + 1, :]
        vecs[P_BQ:P_BQ + 1, lanes] = pbq_b[h:h + 1, :]
        for i, row in enumerate((P_BK, P_BV)):
            vecs[row:row + 1, lanes] = pbkv_b[h, i:i + 1, :]
    for hc in range(hid_chunks):
        span = slice(hc * width, (hc + 1) * width)
        vecs[N_FIXED + hc:N_FIXED + hc + 1, :] = bup_b[span].reshape(1, width)
        vecs[N_FIXED + hid_chunks + hc:N_FIXED + hid_chunks + hc + 1, :] = pbup_b[span].reshape(1, width)
    for slot, row in enumerate((B_Q, B_V)):
        cols[slot] = jnp.transpose(jnp.broadcast_to(vec(row), (LANES, width)))
    qz[...] = jnp.zeros_like(qz)
    abuf[...] = jnp.zeros_like(abuf)
    zbuf[1] = jnp.zeros((BLOCK, width), BF16)
    wait_weight(0)

    def col_bias(slot, lo, size):
        tile = cols[slot, lo:lo + size, :]
        return jnp.concatenate([tile] * (BLOCK // LANES), axis=1)

    def wait_source(j, src):
        pltpu.make_async_copy(images.at[0], xbuf.at[j, src], recv_sem.at[j, src]).wait()

    s_refs = ((s00, s01), (s10, s11))
    p_refs = ((p00, p01), (p10, p11))

    def pool(t, block):
        start = pl.multiple_of((block % nq) * BLOCK, BLOCK)
        kv = dot_t(zbuf[t], wpkv[...])
        score[:, pl.ds(start, BLOCK)] = dot_t(ubuf[...], (kv[:, 0:width] + vec(P_BK)).astype(BF16))
        pvbuf[pl.ds(start, BLOCK), :] = (kv[:, width:2 * width] + vec(P_BV)).astype(BF16)

    def pool_query():
        q16 = jnp.broadcast_to(probe[...], (16, width))
        u = dot_t(q16, wpq[...]) + vec(P_BQ)
        row = lax.broadcasted_iota(jnp.int32, (16, width), 0)
        col = lax.broadcasted_iota(jnp.int32, (16, width), 1)
        ubuf[...] = jnp.where(col // head_dim == row, u, 0.0).astype(BF16)

    def finish_pool(image):
        pool(1, nq - 1)
        s = score[...]
        w = jnp.exp2((s - jnp.max(s, axis=-1, keepdims=True)) * exp_scale)
        a = dot(w.astype(BF16), pvbuf[...]) / jnp.sum(w, axis=-1, keepdims=True)
        row = lax.broadcasted_iota(jnp.int32, (16, width), 0)
        col = lax.broadcasted_iota(jnp.int32, (16, width), 1)
        abuf[pl.ds(image, 1), :] = jnp.sum(jnp.where(col // head_dim == row, a, 0.0), axis=0, keepdims=True)

    def one_image(j, carry):
        def chip_of(k):
            return (own + deltas[k]) % nch

        def enter(k):
            x = xbuf[j, pl.ds(chip_of(k) * 2, 2)].reshape(BLOCK, width)
            for r0 in range(0, BLOCK, 64):
                hbuf[k % 2, r0:r0 + 64, :] = layer_norm(x[r0:r0 + 64].astype(F32), vec(LN1_G), vec(LN1_B)).astype(BF16)

        def project(k):
            tok = pl.multiple_of(chip_of(k) * BLOCK, BLOCK)
            h = hbuf[k % 2]
            for r, size, qt in halves_t(wqkv, 0, width, h):
                qt = (qt + col_bias(0, r, size)).astype(BF16)
                for h0 in range(0, size, head_dim):
                    hd = (r + h0) // head_dim
                    off = (hd % 2) * head_dim
                    qz[hd, off:off + head_dim, pl.ds(tok, BLOCK)] = qt[h0:h0 + head_dim]
            for r, size, v in halves_t(wqkv, 2 * width, width, h):
                vt[r:r + size, pl.ds(tok, BLOCK)] = (v + col_bias(1, r, size)).astype(BF16)
            kbuf[pl.ds(tok, BLOCK), :] = (dot_t(h, wqkv[width:2 * width, :]) + vec(B_K)).astype(BF16)

        def wait_chip(k):
            wait_source(j, chip_of(k) * 2)
            wait_source(j, chip_of(k) * 2 + 1)

        @pl.when(j == 0)
        def _():
            for k in range(nch):
                if k == 1:
                    start_forwards(0)
                    for later in range(1, per):
                        for copy in sends(later):
                            copy.start()
                    for i in (1, *range(3, len(weights))):
                        start_weight(i)
                    wait_weight(2)
                    pool_query()
                wait_chip(k)
                enter(k)
                project(k)

        @pl.when(j > 0)
        def _():
            for k in range(nch):
                wait_chip(k)
            finish_pool(j - 1)
            enter(0)
            for k in range(nch):
                if k + 1 < nch:
                    enter(k + 1)
                project(k)

        def qk(step, slot):
            hp, qb = step // nq, step % nq
            keys = kbuf[:, pl.ds(pl.multiple_of(hp * LANES, LANES), LANES)]
            for hh in (0, 1):
                q = qz[hp * 2 + hh, :, pl.ds(pl.multiple_of(qb * BLOCK, BLOCK), BLOCK)]
                s = dot(keys, q)
                s_refs[slot][hh][...] = s
                mbuf[slot, hh] = jnp.max(s.reshape(tokens // 8, 8, BLOCK), axis=0)

        def softmax_pv(step, slot):
            hp, qb = step // nq, step % nq
            outs = []
            for hh in (0, 1):
                s_ref, p_ref = s_refs[slot][hh], p_refs[slot][hh]
                m = jnp.max(mbuf[slot, hh], axis=0, keepdims=True)
                total = jnp.zeros((8, BLOCK), F32)
                for kc in range(0, tokens, LANES):
                    p = jnp.exp2((s_ref[kc:kc + LANES, :] - m) * exp_scale)
                    total = total + jnp.sum(p.reshape(LANES // 8, 8, BLOCK), axis=0)
                    p_ref[kc:kc + LANES, :] = p.astype(BF16)
                row_sum = jnp.sum(total, axis=0, keepdims=True)
                v = vt[pl.ds(pl.multiple_of(hp * LANES + hh * head_dim, head_dim), head_dim), :]
                outs.append(dot(v, p_ref[...]) * (1.0 / row_sum))
            pair = jnp.transpose(jnp.concatenate(outs, axis=0)).astype(BF16)
            ctx[pl.ds(pl.multiple_of(qb * BLOCK, BLOCK), BLOCK), pl.ds(pl.multiple_of(hp * LANES, LANES), LANES)] = pair

        qk(0, 0)

        def attend(i, c):
            for k in range(UNROLL):
                qk((UNROLL * i + k + 1) % nsteps, (k + 1) % 2)
                softmax_pv(UNROLL * i + k, k % 2)
            return c

        lax.fori_loop(0, nsteps // UNROLL, attend, 0)

        @pl.when(j == 0)
        def _():
            for later in range(1, per):
                start_forwards(later)
            for i in (1, 3, 4, 5):
                wait_weight(i)

        def tail(i, c):
            starts = [pl.multiple_of((2 * i + t) * BLOCK, BLOCK) for t in (0, 1)]

            def resid(t):
                chip = 2 * i + t
                x = xbuf[j, pl.ds(chip * 2, 2)].reshape(BLOCK, width)
                a = dot(ctx[pl.ds(starts[t], BLOCK), :], wout[...])
                rbuf[t] = (x.astype(F32) + a + vec(B_OUT)).astype(BF16)

            def norm(t):
                for r0 in range(0, BLOCK, 64):
                    nbuf[t, r0:r0 + 64, :] = layer_norm(rbuf[t, r0:r0 + 64, :].astype(F32), vec(LN2_G), vec(LN2_B)).astype(BF16)

            def up(t):
                for hc in range(hid_chunks):
                    cols_ = slice(hc * width, (hc + 1) * width)
                    hid[t, :, cols_] = gelu(dot(nbuf[t], wup[:, cols_]) + vec(N_FIXED + hc)).astype(BF16)

            def down(t, row_parts):
                for lo, size, parts in row_parts:
                    rows = slice(lo, lo + size)
                    y = jnp.concatenate([dot(hid[t, rows, :], wdown[:, c0:c1]) for c0, c1 in parts], axis=1)
                    y = (rbuf[t, rows, :].astype(F32) + y + vec(B_DOWN)).astype(BF16)
                    for r0 in range(0, size, 64):
                        zbuf[t, lo + r0:lo + r0 + 64, :] = layer_norm(y[r0:r0 + 64].astype(F32), vec(LNF_G), vec(LNF_B)).astype(BF16)

            whole = [(0, width)]
            row_halves = [(0, BLOCK // 2, whole), (BLOCK // 2, BLOCK // 2, whole)]

            resid(0)
            resid(1)
            pool(1, 2 * i + nq - 1)
            norm(0)
            up(0)
            norm(1)
            up(1)
            down(0, [(0, BLOCK, whole)])
            down(1, row_halves)
            pool(0, 2 * i)
            return c

        lax.fori_loop(0, nq // 2, tail, 0)
        return carry

    lax.fori_loop(0, per, one_image, 0)
    finish_pool(per - 1)

    for i in range(6, len(weights)):
        wait_weight(i)
    o = (dot(abuf[...].astype(BF16), pwout[...]) + vec(P_BOUT)).astype(BF16).astype(F32)
    normed = layer_norm(o, vec(P_LN_G), vec(P_LN_B)).astype(BF16)
    emb = o + vec(P_BDOWN)
    for hc in range(hid_chunks):
        cols_ = slice(hc * width, (hc + 1) * width)
        m = gelu(dot(normed, pwup[:, cols_]) + vec(N_FIXED + hid_chunks + hc)).astype(BF16)
        emb = emb + dot(m, pwdown[cols_, :])
    gath[pl.ds(me, 1)] = emb[0:8][None]

    copies = []
    for s in range(1, n):
        copies.append(pltpu.make_async_remote_copy(
            src_ref=gath.at[me],
            dst_ref=gath.at[me],
            send_sem=gsend_sem.at[s],
            recv_sem=grecv_sem.at[me],
            device_id={"cp": (me + s) % n},
            device_id_type=pl.DeviceIdType.MESH,
        ))
    for copy in copies:
        copy.start()
    for j in range(per):
        for copy in sends(j) + forwards(j):
            copy.wait_send()
    for s in range(1, n):
        src = (me + s) % n
        pltpu.make_async_remote_copy(
            src_ref=gath.at[src], dst_ref=gath.at[src], send_sem=gsend_sem.at[s], recv_sem=grecv_sem.at[src],
            device_id={"cp": src}, device_id_type=pl.DeviceIdType.MESH,
        ).wait_recv()
    for copy in copies:
        copy.wait_send()
    for s in range(n):
        out_ref[s * per:(s + 1) * per, :] = gath[s, 0:per, :]


def solution(mesh):
    n = mesh.shape["cp"]

    def device_step(images, ln1_scale, ln1_bias, w_qkv, b_qkv, w_out, b_out, ln2_scale, ln2_bias, w_up, b_up, w_down, b_down, lnf_scale, lnf_bias, pool_probe, pool_wq, pool_bq, pool_wkv, pool_bkv, pool_wout, pool_bout, pool_ln_scale, pool_ln_bias, pool_w_up, pool_b_up, pool_w_down, pool_b_down):
        count, run, width = images.shape
        heads, head_dim = w_qkv.shape[2:]
        mlp = w_up.shape[1]
        per = count // n
        tokens = n * run
        wqkv_t = jnp.transpose(w_qkv, (1, 2, 3, 0)).reshape(3 * width, width)
        wpkv_t = jnp.transpose(pool_wkv, (1, 2, 3, 0)).reshape(2 * width, width)
        wpq_t = jnp.transpose(pool_wq, (1, 2, 0)).reshape(width, width)
        wout2 = w_out.reshape(width, width)
        pwout2 = pool_wout.reshape(width, width)
        smalls = (ln1_scale, ln1_bias, b_out, ln2_scale, ln2_bias, b_down, lnf_scale, lnf_bias, pool_bout, pool_ln_scale, pool_ln_bias, pool_b_down, b_qkv, pool_bq, jnp.transpose(pool_bkv, (1, 0, 2)), b_up, pool_b_up)
        any_spec = pl.BlockSpec(memory_space=pl.ANY)
        vmem_spec = pl.BlockSpec(memory_space=pltpu.VMEM)
        big = (images, wqkv_t, wout2, w_up, w_down, wpkv_t, wpq_t, pwout2, pool_w_up, pool_w_down)
        scratch = [pltpu.VMEM(w.shape, BF16) for w in big[1:]] + [
            pltpu.VMEM((per, n, run, width), BF16),
            pltpu.VMEM((heads, LANES, tokens), BF16),
            pltpu.VMEM((tokens, width), BF16),
            pltpu.VMEM((width, tokens), BF16),
            *[pltpu.VMEM((tokens, BLOCK), F32) for _ in range(4)],
            *[pltpu.VMEM((tokens, BLOCK), BF16) for _ in range(4)],
            pltpu.VMEM((2, 2, 8, BLOCK), F32),
            pltpu.VMEM((tokens, width), BF16),
            pltpu.VMEM((2, BLOCK, width), BF16),
            pltpu.VMEM((2, BLOCK, width), BF16),
            pltpu.VMEM((2, BLOCK, width), BF16),
            pltpu.VMEM((2, BLOCK, mlp), BF16),
            pltpu.VMEM((2, BLOCK, width), BF16),
            pltpu.VMEM((16, tokens), F32),
            pltpu.VMEM((tokens, width), BF16),
            pltpu.VMEM((16, width), BF16),
            pltpu.VMEM((2, width, LANES), F32),
            pltpu.VMEM((16, width), F32),
            pltpu.VMEM((n, 8, width), F32),
            pltpu.VMEM((per, 2, run, width), BF16),
            pltpu.VMEM((N_FIXED + 2 * mlp // width, width), F32),
            pltpu.VMEM(pool_probe.shape, BF16),
            *[pltpu.VMEM(v.shape, F32) for v in smalls],
            pltpu.SemaphoreType.DMA((per, n)),
            pltpu.SemaphoreType.DMA((per, n)),
            pltpu.SemaphoreType.DMA((per, 2)),
            pltpu.SemaphoreType.DMA((per, 2)),
            pltpu.SemaphoreType.DMA((len(big) - 1,)),
            pltpu.SemaphoreType.DMA((n,)),
            pltpu.SemaphoreType.DMA((n,)),
            pltpu.SemaphoreType.DMA((N_SMALL + 1,)),
        ]
        return pl.pallas_call(
            functools.partial(kernel, (n, per, heads, head_dim, width, mlp)),
            out_shape=jax.ShapeDtypeStruct((count, width), F32),
            in_specs=[any_spec] * (len(big) + len(smalls) + 1),
            out_specs=vmem_spec,
            scratch_shapes=scratch,
            compiler_params=pltpu.CompilerParams(collective_id=0, has_side_effects=True, vmem_limit_bytes=67043328),
            name="encoder_pool",
        )(*big, *smalls, pool_probe)

    in_specs = (P("dp", "cp", None),) + (P(),) * 27
    return jax.shard_map(device_step, mesh=mesh, in_specs=in_specs, out_specs=P("dp", None), check_vma=False)
```

```python
import functools
import math

import jax
import jax.numpy as jnp
from jax import lax
from jax.experimental import pallas as pl
from jax.experimental.pallas import tpu as pltpu
from jax.sharding import PartitionSpec as P

EPSILON = 1e-6
LANES = 128
BLOCK = 256
UNROLL = 12
F32 = jnp.float32
BF16 = jnp.bfloat16

(LN1_G, LN1_B, B_OUT, LN2_G, LN2_B, B_DOWN, LNF_G, LNF_B, P_BOUT, P_LN_G, P_LN_B, P_BDOWN, B_Q, B_K, B_V, P_BQ, P_BK, P_BV) = range(18)
N_FIXED = 18
N_SMALL = 17


def layer_norm(values, ln_gain, ln_shift):
    row_mean = jnp.mean(values, axis=-1, keepdims=True)
    centered = values - row_mean
    variance = jnp.mean(centered * centered, axis=-1, keepdims=True)
    return centered * lax.rsqrt(variance + EPSILON) * ln_gain + ln_shift


def gelu(x):
    return jax.nn.gelu(x, approximate=True)


def dot(a, b):
    return lax.dot_general(a, b, (((1,), (0,)), ((), ())), preferred_element_type=F32)


def dot_t(a, b):
    return lax.dot_general(a, b, (((1,), (1,)), ((), ())), preferred_element_type=F32)


def halves_t(a_ref, lo, size, b):
    half = size // 2
    return [(r, half, dot_t(a_ref[lo + r:lo + r + half, :], b)) for r in (0, half)]


def kernel(cfg, images, wqkv_h, wout_h, wup_h, wdown_h, wpkv_h, wpq_h, pwout_h, pwup_h, pwdown_h, *rest):
    n, per, heads, head_dim, width, mlp = cfg
    smalls = rest[:N_SMALL]
    (probe_h, out_ref,
           wqkv, wout, wup, wdown, wpkv, wpq, pwout, pwup, pwdown,
           xbuf, qz, kbuf, vt, s00, s01, s10, s11, mbuf, ctx, hbuf, rbuf, nbuf, hid, zbuf,
           score, pvbuf, ubuf, cols, abuf, gath, rel, vecs, probe, *tail_refs) = rest[N_SMALL:]
    small_bufs = tail_refs[:N_SMALL]
    send_sem, recv_sem, rel_sem, fwd_sem, w_sem, gsend_sem, grecv_sem, v_sem = tail_refs[N_SMALL:]
    run = images.shape[1]
    tokens = n * run
    nch = n // 2
    hid_chunks = mlp // width
    pairs = heads // 2
    nq = tokens // BLOCK
    nsteps = pairs * nq
    exp_scale = math.log2(math.e) * head_dim ** -0.5
    me = lax.axis_index("cp")
    own = me // 2
    core = me % 2

    def vec(i):
        return vecs[i:i + 1, :]

    def weight_copy(i, src, dst):
        return pltpu.make_async_copy(src, dst, w_sem.at[i])

    weights = [(wqkv_h, wqkv), (wout_h, wout), (wpq_h, wpq), (wup_h, wup), (wdown_h, wdown), (wpkv_h, wpkv), (pwout_h, pwout), (pwup_h, pwup), (pwdown_h, pwdown)]

    def start_weight(i):
        weight_copy(i, *weights[i]).start()

    def wait_weight(i):
        weight_copy(i, *weights[i]).wait()

    def local_copy(j):
        return pltpu.make_async_copy(images.at[me * per + j], xbuf.at[j, me], recv_sem.at[j, me])

    deltas = [0]
    for d in range(1, nch // 2 + 1):
        deltas.append(d)
        if nch - d != d:
            deltas.append(nch - d)

    def remote(src, dst, send, recv, device):
        return pltpu.make_async_remote_copy(
            src_ref=src, dst_ref=dst, send_sem=send, recv_sem=recv, device_id={"cp": device}, device_id_type=pl.DeviceIdType.MESH)

    relayed = nch == 4

    def chip_core(delta, c):
        return ((own + delta + nch) % nch) * 2 + c

    def sends(j):
        copies = []

        def add(block, dst, recv, device):
            copies.append(remote(images.at[block * per + j], dst, send_sem.at[j, len(copies)], recv, device))

        add(chip_core(0, 1 - core), xbuf.at[j, me], recv_sem.at[j, me], chip_core(0, 1 - core))
        for up in (0, 1) if relayed else ():
            add(chip_core(2, up), rel.at[j, up], rel_sem.at[j, up], chip_core(1 - 2 * up, core))
        for delta in deltas:
            for cc in (0, 1):
                if delta == 0 or (relayed and delta == 2):
                    continue
                dst = chip_core(delta, (core + cc) % 2)
                add(dst, xbuf.at[j, me], recv_sem.at[j, me], dst)
        return copies

    def forwards(j):
        copies = []
        for up in (0, 1) if relayed else ():
            source = chip_core(2 * up - 1, core)
            copies.append(remote(rel.at[j, up], xbuf.at[j, source], fwd_sem.at[j, up], recv_sem.at[j, source], chip_core(1 - 2 * up, up)))
        return copies

    def start_forwards(j):
        for up, copy in enumerate(forwards(j)):
            pltpu.make_async_copy(images.at[0], rel.at[j, up], rel_sem.at[j, up]).wait()
            copy.start()

    small_copies = [pltpu.make_async_copy(src, dst, v_sem.at[i]) for i, (src, dst) in enumerate(zip((*smalls, probe_h), (*small_bufs, probe)))]
    start_weight(0)
    for j in range(per):
        local_copy(j).start()
    for copy in small_copies:
        copy.start()

    barrier = pltpu.get_barrier_semaphore()
    for s in range(1, n):
        pl.semaphore_signal(barrier, inc=1, device_id={"cp": (me + s) % n}, device_id_type=pl.DeviceIdType.MESH)
    pl.semaphore_wait(barrier, n - 1)

    for copy in sends(0):
        copy.start()
    for later in range(1, per):
        sends(later)[0].start()
    start_weight(2)

    for copy in small_copies:
        copy.wait()
    for i, buf in enumerate(small_bufs[:12]):
        vecs[i:i + 1, :] = buf[...].reshape(1, width)
    bqkv_b, pbq_b, pbkv_b, bup_b, pbup_b = small_bufs[12:]
    for h in range(heads):
        lanes = slice(h * head_dim, (h + 1) * head_dim)
        for i, row in enumerate((B_Q, B_K, B_V)):
            vecs[row:row + 1, lanes] = bqkv_b[i, h:h + 1, :]
        vecs[P_BQ:P_BQ + 1, lanes] = pbq_b[h:h + 1, :]
        for i, row in enumerate((P_BK, P_BV)):
            vecs[row:row + 1, lanes] = pbkv_b[h, i:i + 1, :]
    for hc in range(hid_chunks):
        span = slice(hc * width, (hc + 1) * width)
        vecs[N_FIXED + hc:N_FIXED + hc + 1, :] = bup_b[span].reshape(1, width)
        vecs[N_FIXED + hid_chunks + hc:N_FIXED + hid_chunks + hc + 1, :] = pbup_b[span].reshape(1, width)
    for slot, row in enumerate((B_Q, B_V)):
        cols[slot] = jnp.transpose(jnp.broadcast_to(vec(row), (LANES, width)))
    qz[...] = jnp.zeros_like(qz)
    abuf[...] = jnp.zeros_like(abuf)
    zbuf[1] = jnp.zeros((BLOCK, width), BF16)
    wait_weight(0)

    def col_bias(slot, lo, size):
        tile = cols[slot, lo:lo + size, :]
        return jnp.concatenate([tile] * (BLOCK // LANES), axis=1)

    def wait_source(j, src):
        pltpu.make_async_copy(images.at[0], xbuf.at[j, src], recv_sem.at[j, src]).wait()

    s_refs = ((s00, s01), (s10, s11))

    def pool(t, block):
        start = pl.multiple_of((block % nq) * BLOCK, BLOCK)
        kv = dot_t(zbuf[t], wpkv[...])
        score[:, pl.ds(start, BLOCK)] = dot_t(ubuf[...], (kv[:, 0:width] + vec(P_BK)).astype(BF16))
        pvbuf[pl.ds(start, BLOCK), :] = (kv[:, width:2 * width] + vec(P_BV)).astype(BF16)

    def pool_query():
        q16 = jnp.broadcast_to(probe[...], (16, width))
        u = dot_t(q16, wpq[...]) + vec(P_BQ)
        row = lax.broadcasted_iota(jnp.int32, (16, width), 0)
        col = lax.broadcasted_iota(jnp.int32, (16, width), 1)
        ubuf[...] = jnp.where(col // head_dim == row, u, 0.0).astype(BF16)

    def finish_pool(image):
        pool(1, nq - 1)
        s = score[...]
        w = jnp.exp2((s - jnp.max(s, axis=-1, keepdims=True)) * exp_scale)
        a = dot(w.astype(BF16), pvbuf[...]) / jnp.sum(w, axis=-1, keepdims=True)
        row = lax.broadcasted_iota(jnp.int32, (16, width), 0)
        col = lax.broadcasted_iota(jnp.int32, (16, width), 1)
        abuf[pl.ds(image, 1), :] = jnp.sum(jnp.where(col // head_dim == row, a, 0.0), axis=0, keepdims=True)

    def one_image(j, carry):
        def chip_of(k):
            return (own + deltas[k]) % nch

        def enter(im, k):
            x = xbuf[im, pl.ds(chip_of(k) * 2, 2)].reshape(BLOCK, width)
            for r0 in range(0, BLOCK, 64):
                hbuf[k % 2, r0:r0 + 64, :] = layer_norm(x[r0:r0 + 64].astype(F32), vec(LN1_G), vec(LN1_B)).astype(BF16)

        def project(im, k):
            tok = pl.multiple_of(chip_of(k) * BLOCK, BLOCK)
            h = hbuf[k % 2]
            for r, size, qt in halves_t(wqkv, 0, width, h):
                qt = (qt + col_bias(0, r, size)).astype(BF16)
                for h0 in range(0, size, head_dim):
                    hd = (r + h0) // head_dim
                    off = (hd % 2) * head_dim
                    qz[im, hd, off:off + head_dim, pl.ds(tok, BLOCK)] = qt[h0:h0 + head_dim]
            for r, size, v in halves_t(wqkv, 2 * width, width, h):
                vt[im, r:r + size, pl.ds(tok, BLOCK)] = (v + col_bias(1, r, size)).astype(BF16)
            kbuf[im, pl.ds(tok, BLOCK), :] = (dot_t(h, wqkv[width:2 * width, :]) + vec(B_K)).astype(BF16)

        def wait_chip(im, k):
            wait_source(im, chip_of(k) * 2)
            wait_source(im, chip_of(k) * 2 + 1)

        @pl.when(j == 0)
        def _():
            for k in range(nch):
                if k == 1:
                    start_forwards(0)
                    for later in range(1, per):
                        for copy in sends(later)[1:]:
                            copy.start()
                    for i in (1, *range(3, len(weights))):
                        start_weight(i)
                    wait_weight(2)
                    pool_query()
                    for later in range(1, per):
                        wait_chip(later, 0)
                        enter(later, 0)
                        project(later, 0)
                wait_chip(0, k)
                enter(0, k)
                project(0, k)

        @pl.when(j > 0)
        def _():
            for k in range(1, nch):
                wait_chip(j, k)
            finish_pool(j - 1)
            enter(j, 1)
            for k in range(1, nch):
                if k + 1 < nch:
                    enter(j, k + 1)
                project(j, k)

        def qk(step, slot):
            hp, qb = step // nq, step % nq
            keys = kbuf[j, :, pl.ds(pl.multiple_of(hp * LANES, LANES), LANES)]
            for hh in (0, 1):
                q = qz[j, hp * 2 + hh, :, pl.ds(pl.multiple_of(qb * BLOCK, BLOCK), BLOCK)]
                s = dot(keys, q)
                s_refs[slot][hh][...] = s
                mbuf[slot, hh] = jnp.max(s.reshape(tokens // 8, 8, BLOCK), axis=0)

        def softmax_pv(step, slot):
            hp, qb = step // nq, step % nq
            outs = []
            for hh in (0, 1):
                s_ref = s_refs[slot][hh]
                parts = []
                m = jnp.max(mbuf[slot, hh], axis=0, keepdims=True)
                total = jnp.zeros((8, BLOCK), F32)
                for kc in range(0, tokens, LANES):
                    p = jnp.exp2((s_ref[kc:kc + LANES, :] - m) * exp_scale)
                    total = total + jnp.sum(p.reshape(LANES // 8, 8, BLOCK), axis=0)
                    parts.append(p.astype(BF16))
                row_sum = jnp.sum(total, axis=0, keepdims=True)
                v = vt[j, pl.ds(pl.multiple_of(hp * LANES + hh * head_dim, head_dim), head_dim), :]
                outs.append(dot(v, jnp.concatenate(parts, axis=0)) * (1.0 / row_sum))
            pair = jnp.transpose(jnp.concatenate(outs, axis=0)).astype(BF16)
            ctx[pl.ds(pl.multiple_of(qb * BLOCK, BLOCK), BLOCK), pl.ds(pl.multiple_of(hp * LANES, LANES), LANES)] = pair

        qk(0, 0)

        def attend(i, c):
            for k in range(UNROLL):
                qk((UNROLL * i + k + 1) % nsteps, (k + 1) % 2)
                softmax_pv(UNROLL * i + k, k % 2)
            return c

        lax.fori_loop(0, nsteps // UNROLL, attend, 0)

        @pl.when(j == 0)
        def _():
            for later in range(1, per):
                start_forwards(later)
            for i in (1, 3, 4, 5):
                wait_weight(i)

        def tail(i, c):
            starts = [pl.multiple_of((2 * i + t) * BLOCK, BLOCK) for t in (0, 1)]

            def resid(t):
                chip = 2 * i + t
                x = xbuf[j, pl.ds(chip * 2, 2)].reshape(BLOCK, width)
                a = dot(ctx[pl.ds(starts[t], BLOCK), :], wout[...])
                rbuf[t] = (x.astype(F32) + a + vec(B_OUT)).astype(BF16)

            def norm(t):
                for r0 in range(0, BLOCK, 64):
                    nbuf[t, r0:r0 + 64, :] = layer_norm(rbuf[t, r0:r0 + 64, :].astype(F32), vec(LN2_G), vec(LN2_B)).astype(BF16)

            def up(t):
                for hc in range(hid_chunks):
                    cols_ = slice(hc * width, (hc + 1) * width)
                    hid[t, :, cols_] = gelu(dot(nbuf[t], wup[:, cols_]) + vec(N_FIXED + hc)).astype(BF16)

            def down(t, row_parts):
                for lo, size, parts in row_parts:
                    rows = slice(lo, lo + size)
                    y = jnp.concatenate([dot(hid[t, rows, :], wdown[:, c0:c1]) for c0, c1 in parts], axis=1)
                    y = (rbuf[t, rows, :].astype(F32) + y + vec(B_DOWN)).astype(BF16)
                    for r0 in range(0, size, 64):
                        zbuf[t, lo + r0:lo + r0 + 64, :] = layer_norm(y[r0:r0 + 64].astype(F32), vec(LNF_G), vec(LNF_B)).astype(BF16)

            whole = [(0, width)]
            row_halves = [(0, BLOCK // 2, whole), (BLOCK // 2, BLOCK // 2, whole)]

            resid(0)
            resid(1)
            pool(1, 2 * i + nq - 1)
            norm(0)
            up(0)
            norm(1)
            up(1)
            down(0, [(0, BLOCK, whole)])
            down(1, row_halves)
            pool(0, 2 * i)
            return c

        lax.fori_loop(0, nq // 2, tail, 0)
        return carry

    lax.fori_loop(0, per, one_image, 0)
    finish_pool(per - 1)

    for i in range(6, len(weights)):
        wait_weight(i)
    o = (dot(abuf[...].astype(BF16), pwout[...]) + vec(P_BOUT)).astype(BF16).astype(F32)
    normed = layer_norm(o, vec(P_LN_G), vec(P_LN_B)).astype(BF16)
    emb = o + vec(P_BDOWN)
    for hc in range(hid_chunks):
        cols_ = slice(hc * width, (hc + 1) * width)
        m = gelu(dot(normed, pwup[:, cols_]) + vec(N_FIXED + hid_chunks + hc)).astype(BF16)
        emb = emb + dot(m, pwdown[cols_, :])
    gath[pl.ds(me, 1)] = emb[0:8][None]

    copies = []
    for s in range(1, n):
        copies.append(pltpu.make_async_remote_copy(
            src_ref=gath.at[me],
            dst_ref=gath.at[me],
            send_sem=gsend_sem.at[s],
            recv_sem=grecv_sem.at[me],
            device_id={"cp": (me + s) % n},
            device_id_type=pl.DeviceIdType.MESH,
        ))
    for copy in copies:
        copy.start()
    for j in range(per):
        for copy in sends(j) + forwards(j):
            copy.wait_send()
    for s in range(1, n):
        src = (me + s) % n
        pltpu.make_async_remote_copy(
            src_ref=gath.at[src], dst_ref=gath.at[src], send_sem=gsend_sem.at[s], recv_sem=grecv_sem.at[src],
            device_id={"cp": src}, device_id_type=pl.DeviceIdType.MESH,
        ).wait_recv()
    for copy in copies:
        copy.wait_send()
    for s in range(n):
        out_ref[s * per:(s + 1) * per, :] = gath[s, 0:per, :]


def solution(mesh):
    n = mesh.shape["cp"]

    def device_step(images, ln1_scale, ln1_bias, w_qkv, b_qkv, w_out, b_out, ln2_scale, ln2_bias, w_up, b_up, w_down, b_down, lnf_scale, lnf_bias, pool_probe, pool_wq, pool_bq, pool_wkv, pool_bkv, pool_wout, pool_bout, pool_ln_scale, pool_ln_bias, pool_w_up, pool_b_up, pool_w_down, pool_b_down):
        count, run, width = images.shape
        heads, head_dim = w_qkv.shape[2:]
        mlp = w_up.shape[1]
        per = count // n
        tokens = n * run
        wqkv_t = jnp.transpose(w_qkv, (1, 2, 3, 0)).reshape(3 * width, width)
        wpkv_t = jnp.transpose(pool_wkv, (1, 2, 3, 0)).reshape(2 * width, width)
        wpq_t = jnp.transpose(pool_wq, (1, 2, 0)).reshape(width, width)
        wout2 = w_out.reshape(width, width)
        pwout2 = pool_wout.reshape(width, width)
        smalls = (ln1_scale, ln1_bias, b_out, ln2_scale, ln2_bias, b_down, lnf_scale, lnf_bias, pool_bout, pool_ln_scale, pool_ln_bias, pool_b_down, b_qkv, pool_bq, jnp.transpose(pool_bkv, (1, 0, 2)), b_up, pool_b_up)
        any_spec = pl.BlockSpec(memory_space=pl.ANY)
        vmem_spec = pl.BlockSpec(memory_space=pltpu.VMEM)
        big = (images, wqkv_t, wout2, w_up, w_down, wpkv_t, wpq_t, pwout2, pool_w_up, pool_w_down)
        scratch = [pltpu.VMEM(w.shape, BF16) for w in big[1:]] + [
            pltpu.VMEM((per, n, run, width), BF16),
            pltpu.VMEM((per, heads, LANES, tokens), BF16),
            pltpu.VMEM((per, tokens, width), BF16),
            pltpu.VMEM((per, width, tokens), BF16),
            *[pltpu.VMEM((tokens, BLOCK), F32) for _ in range(4)],
            pltpu.VMEM((2, 2, 8, BLOCK), F32),
            pltpu.VMEM((tokens, width), BF16),
            pltpu.VMEM((2, BLOCK, width), BF16),
            pltpu.VMEM((2, BLOCK, width), BF16),
            pltpu.VMEM((2, BLOCK, width), BF16),
            pltpu.VMEM((2, BLOCK, mlp), BF16),
            pltpu.VMEM((2, BLOCK, width), BF16),
            pltpu.VMEM((16, tokens), F32),
            pltpu.VMEM((tokens, width), BF16),
            pltpu.VMEM((16, width), BF16),
            pltpu.VMEM((2, width, LANES), F32),
            pltpu.VMEM((16, width), F32),
            pltpu.VMEM((n, 8, width), F32),
            pltpu.VMEM((per, 2, run, width), BF16),
            pltpu.VMEM((N_FIXED + 2 * mlp // width, width), F32),
            pltpu.VMEM(pool_probe.shape, BF16),
            *[pltpu.VMEM(v.shape, F32) for v in smalls],
            pltpu.SemaphoreType.DMA((per, n)),
            pltpu.SemaphoreType.DMA((per, n)),
            pltpu.SemaphoreType.DMA((per, 2)),
            pltpu.SemaphoreType.DMA((per, 2)),
            pltpu.SemaphoreType.DMA((len(big) - 1,)),
            pltpu.SemaphoreType.DMA((n,)),
            pltpu.SemaphoreType.DMA((n,)),
            pltpu.SemaphoreType.DMA((N_SMALL + 1,)),
        ]
        return pl.pallas_call(
            functools.partial(kernel, (n, per, heads, head_dim, width, mlp)),
            out_shape=jax.ShapeDtypeStruct((count, width), F32),
            in_specs=[any_spec] * (len(big) + len(smalls) + 1),
            out_specs=vmem_spec,
            scratch_shapes=scratch,
            compiler_params=pltpu.CompilerParams(collective_id=0, has_side_effects=True, vmem_limit_bytes=67043328),
            name="encoder_pool",
        )(*big, *smalls, pool_probe)

    in_specs = (P("dp", "cp", None),) + (P(),) * 27
    return jax.shard_map(device_step, mesh=mesh, in_specs=in_specs, out_specs=P("dp", None), check_vma=False)
```

```python
import functools
import math

import jax
import jax.numpy as jnp
from jax import lax
from jax.experimental import pallas as pl
from jax.experimental.pallas import tpu as pltpu
from jax.sharding import PartitionSpec as P

EPSILON = 1e-6
LANES = 128
BLOCK = 256
F32 = jnp.float32
BF16 = jnp.bfloat16

(LN1_G, LN1_B, B_OUT, LN2_G, LN2_B, B_DOWN, LNF_G, LNF_B, P_BOUT, P_LN_G, P_LN_B, P_BDOWN, B_Q, B_K, B_V, P_BQ, P_BK, P_BV) = range(18)
N_FIXED = 18
N_SMALL = 17


def layer_norm(values, ln_gain, ln_shift):
    row_mean = jnp.mean(values, axis=-1, keepdims=True)
    centered = values - row_mean
    variance = jnp.mean(centered * centered, axis=-1, keepdims=True)
    return centered * lax.rsqrt(variance + EPSILON) * ln_gain + ln_shift


def gelu(x):
    return jax.nn.gelu(x, approximate=True)


def dot(a, b):
    return lax.dot_general(a, b, (((1,), (0,)), ((), ())), preferred_element_type=F32)


def dot_t(a, b):
    return lax.dot_general(a, b, (((1,), (1,)), ((), ())), preferred_element_type=F32)


def halves_t(a_ref, lo, size, b):
    half = size // 2
    return [(r, half, dot_t(a_ref[lo + r:lo + r + half, :], b)) for r in (0, half)]


def kernel(cfg, images, wqkv_h, wout_h, wup_h, wdown_h, wpkv_h, wpq_h, pwout_h, pwup_h, pwdown_h, *rest):
    n, per, heads, head_dim, width, mlp = cfg
    smalls = rest[:N_SMALL]
    (probe_h, out_ref,
           wqkv, wout, wup, wdown, wpkv, wpq, pwout, pwup, pwdown,
           xbuf, qz, kbuf, vt, s00, s01, s10, s11, mbuf, ctx, hbuf, rbuf, nbuf, hid, zbuf,
           score, pvbuf, ubuf, cols, abuf, gath, rel, vecs, probe, *tail_refs) = rest[N_SMALL:]
    small_bufs = tail_refs[:N_SMALL]
    send_sem, recv_sem, rel_sem, fwd_sem, w_sem, gsend_sem, grecv_sem, v_sem = tail_refs[N_SMALL:]
    run = images.shape[1]
    tokens = n * run
    nch = n // 2
    hid_chunks = mlp // width
    pairs = heads // 2
    nq = tokens // BLOCK
    nsteps = pairs * nq
    exp_scale = math.log2(math.e) * head_dim ** -0.5
    me = lax.axis_index("cp")
    own = me // 2
    core = me % 2

    def vec(i):
        return vecs[i:i + 1, :]

    def weight_copy(i, src, dst):
        return pltpu.make_async_copy(src, dst, w_sem.at[i])

    weights = [(wqkv_h, wqkv), (wout_h, wout), (wpq_h, wpq), (wup_h, wup), (wdown_h, wdown), (wpkv_h, wpkv), (pwout_h, pwout), (pwup_h, pwup), (pwdown_h, pwdown)]

    def start_weight(i):
        weight_copy(i, *weights[i]).start()

    def wait_weight(i):
        weight_copy(i, *weights[i]).wait()

    def local_copy(j):
        return pltpu.make_async_copy(images.at[me * per + j], xbuf.at[j, me], recv_sem.at[j, me])

    deltas = [0]
    for d in range(1, nch // 2 + 1):
        deltas.append(d)
        if nch - d != d:
            deltas.append(nch - d)

    def remote(src, dst, send, recv, device):
        return pltpu.make_async_remote_copy(
            src_ref=src, dst_ref=dst, send_sem=send, recv_sem=recv, device_id={"cp": device}, device_id_type=pl.DeviceIdType.MESH)

    relayed = nch == 4

    def chip_core(delta, c):
        return ((own + delta + nch) % nch) * 2 + c

    def sends(j):
        copies = []

        def add(block, dst, recv, device):
            copies.append(remote(images.at[block * per + j], dst, send_sem.at[j, len(copies)], recv, device))

        add(chip_core(0, 1 - core), xbuf.at[j, me], recv_sem.at[j, me], chip_core(0, 1 - core))
        for up in (0, 1) if relayed else ():
            add(chip_core(2, up), rel.at[j, up], rel_sem.at[j, up], chip_core(1 - 2 * up, core))
        for delta in deltas:
            for cc in (0, 1):
                if delta == 0 or (relayed and delta == 2):
                    continue
                dst = chip_core(delta, (core + cc) % 2)
                add(dst, xbuf.at[j, me], recv_sem.at[j, me], dst)
        return copies

    def forwards(j):
        copies = []
        for up in (0, 1) if relayed else ():
            source = chip_core(2 * up - 1, core)
            copies.append(remote(rel.at[j, up], xbuf.at[j, source], fwd_sem.at[j, up], recv_sem.at[j, source], chip_core(1 - 2 * up, up)))
        return copies

    def start_forwards(j):
        for up, copy in enumerate(forwards(j)):
            pltpu.make_async_copy(images.at[0], rel.at[j, up], rel_sem.at[j, up]).wait()
            copy.start()

    small_copies = [pltpu.make_async_copy(src, dst, v_sem.at[i]) for i, (src, dst) in enumerate(zip((*smalls, probe_h), (*small_bufs, probe)))]
    start_weight(0)
    for j in range(per):
        local_copy(j).start()
    for copy in small_copies:
        copy.start()

    barrier = pltpu.get_barrier_semaphore()
    for s in range(1, n):
        pl.semaphore_signal(barrier, inc=1, device_id={"cp": (me + s) % n}, device_id_type=pl.DeviceIdType.MESH)
    pl.semaphore_wait(barrier, n - 1)

    for copy in sends(0):
        copy.start()
    for later in range(1, per):
        sends(later)[0].start()
    start_weight(2)

    for copy in small_copies:
        copy.wait()
    for i, buf in enumerate(small_bufs[:12]):
        vecs[i:i + 1, :] = buf[...].reshape(1, width)
    bqkv_b, pbq_b, pbkv_b, bup_b, pbup_b = small_bufs[12:]
    for h in range(heads):
        lanes = slice(h * head_dim, (h + 1) * head_dim)
        for i, row in enumerate((B_Q, B_K, B_V)):
            vecs[row:row + 1, lanes] = bqkv_b[i, h:h + 1, :]
        vecs[P_BQ:P_BQ + 1, lanes] = pbq_b[h:h + 1, :]
        for i, row in enumerate((P_BK, P_BV)):
            vecs[row:row + 1, lanes] = pbkv_b[h, i:i + 1, :]
    for hc in range(hid_chunks):
        span = slice(hc * width, (hc + 1) * width)
        vecs[N_FIXED + hc:N_FIXED + hc + 1, :] = bup_b[span].reshape(1, width)
        vecs[N_FIXED + hid_chunks + hc:N_FIXED + hid_chunks + hc + 1, :] = pbup_b[span].reshape(1, width)
    for slot, row in enumerate((B_Q, B_V)):
        cols[slot] = jnp.transpose(jnp.broadcast_to(vec(row), (LANES, width)))
    qz[...] = jnp.zeros_like(qz)
    abuf[...] = jnp.zeros_like(abuf)
    zbuf[1] = jnp.zeros((BLOCK, width), BF16)
    wait_weight(0)

    def col_bias(slot, lo, size):
        tile = cols[slot, lo:lo + size, :]
        return jnp.concatenate([tile] * (BLOCK // LANES), axis=1)

    def wait_source(j, src):
        pltpu.make_async_copy(images.at[0], xbuf.at[j, src], recv_sem.at[j, src]).wait()

    s_refs = ((s00, s01), (s10, s11))

    def pool(t, block):
        start = pl.multiple_of((block % nq) * BLOCK, BLOCK)
        kv = dot_t(zbuf[t], wpkv[...])
        score[:, pl.ds(start, BLOCK)] = dot_t(ubuf[...], (kv[:, 0:width] + vec(P_BK)).astype(BF16))
        pvbuf[pl.ds(start, BLOCK), :] = (kv[:, width:2 * width] + vec(P_BV)).astype(BF16)

    def pool_query():
        q16 = jnp.broadcast_to(probe[...], (16, width))
        u = dot_t(q16, wpq[...]) + vec(P_BQ)
        row = lax.broadcasted_iota(jnp.int32, (16, width), 0)
        col = lax.broadcasted_iota(jnp.int32, (16, width), 1)
        ubuf[...] = jnp.where(col // head_dim == row, u, 0.0).astype(BF16)

    def finish_pool(image):
        pool(1, nq - 1)
        s = score[...]
        w = jnp.exp2((s - jnp.max(s, axis=-1, keepdims=True)) * exp_scale)
        a = dot(w.astype(BF16), pvbuf[...]) / jnp.sum(w, axis=-1, keepdims=True)
        row = lax.broadcasted_iota(jnp.int32, (16, width), 0)
        col = lax.broadcasted_iota(jnp.int32, (16, width), 1)
        abuf[pl.ds(image, 1), :] = jnp.sum(jnp.where(col // head_dim == row, a, 0.0), axis=0, keepdims=True)

    def one_image(j, carry):
        def chip_of(k):
            return (own + deltas[k]) % nch

        def enter(im, k):
            x = xbuf[im, pl.ds(chip_of(k) * 2, 2)].reshape(BLOCK, width)
            for r0 in range(0, BLOCK, 64):
                hbuf[k % 2, r0:r0 + 64, :] = layer_norm(x[r0:r0 + 64].astype(F32), vec(LN1_G), vec(LN1_B)).astype(BF16)

        def project(im, k):
            tok = pl.multiple_of(chip_of(k) * BLOCK, BLOCK)
            h = hbuf[k % 2]
            for r, size, qt in halves_t(wqkv, 0, width, h):
                qt = (qt + col_bias(0, r, size)).astype(BF16)
                for h0 in range(0, size, head_dim):
                    hd = (r + h0) // head_dim
                    off = (hd % 2) * head_dim
                    qz[im, hd, off:off + head_dim, pl.ds(tok, BLOCK)] = qt[h0:h0 + head_dim]
            for r, size, v in halves_t(wqkv, 2 * width, width, h):
                vt[im, r:r + size, pl.ds(tok, BLOCK)] = (v + col_bias(1, r, size)).astype(BF16)
            kbuf[im, pl.ds(tok, BLOCK), :] = (dot_t(h, wqkv[width:2 * width, :]) + vec(B_K)).astype(BF16)

        def wait_chip(im, k):
            wait_source(im, chip_of(k) * 2)
            wait_source(im, chip_of(k) * 2 + 1)

        @pl.when(j == 0)
        def _():
            for k in range(nch):
                if k == 1:
                    start_forwards(0)
                    for later in range(1, per):
                        for copy in sends(later)[1:]:
                            copy.start()
                    for i in (1, *range(3, len(weights))):
                        start_weight(i)
                    wait_weight(2)
                    pool_query()
                    for later in range(1, per):
                        wait_chip(later, 0)
                        enter(later, 0)
                        project(later, 0)
                wait_chip(0, k)
                enter(0, k)
                project(0, k)

        @pl.when(j > 0)
        def _():
            for k in range(1, nch):
                wait_chip(j, k)
            finish_pool(j - 1)
            enter(j, 1)
            for k in range(1, nch):
                if k + 1 < nch:
                    enter(j, k + 1)
                project(j, k)

        def qk(step, slot):
            hp, qb = step // nq, step % nq
            keys = kbuf[j, :, pl.ds(hp * LANES, LANES)]
            for hh in (0, 1):
                q = qz[j, hp * 2 + hh, :, pl.ds(qb * BLOCK, BLOCK)]
                s = dot(keys, q)
                s_refs[slot][hh][...] = s
                mbuf[slot, hh] = jnp.max(s.reshape(tokens // 8, 8, BLOCK), axis=0)

        def softmax_pv(step, slot):
            hp, qb = step // nq, step % nq
            outs = []
            for hh in (0, 1):
                s_ref = s_refs[slot][hh]
                parts = []
                m = jnp.max(mbuf[slot, hh], axis=0, keepdims=True)
                total = jnp.zeros((8, BLOCK), F32)
                for kc in range(0, tokens, LANES):
                    p = jnp.exp2((s_ref[kc:kc + LANES, :] - m) * exp_scale)
                    total = total + jnp.sum(p.reshape(LANES // 8, 8, BLOCK), axis=0)
                    parts.append(p.astype(BF16))
                row_sum = jnp.sum(total, axis=0, keepdims=True)
                v = vt[j, pl.ds(hp * LANES + hh * head_dim, head_dim), :]
                outs.append(dot(v, jnp.concatenate(parts, axis=0)) * (1.0 / row_sum))
            pair = jnp.transpose(jnp.concatenate(outs, axis=0)).astype(BF16)
            ctx[pl.ds(qb * BLOCK, BLOCK), pl.ds(hp * LANES, LANES)] = pair

        qk(0, 0)
        for k in range(nsteps):
            if k + 1 < nsteps:
                qk(k + 1, (k + 1) % 2)
            softmax_pv(k, k % 2)

        @pl.when(j == 0)
        def _():
            for later in range(1, per):
                start_forwards(later)
            for i in (1, 3, 4, 5):
                wait_weight(i)

        def tail(i, c):
            starts = [pl.multiple_of((2 * i + t) * BLOCK, BLOCK) for t in (0, 1)]

            def resid(t):
                chip = 2 * i + t
                x = xbuf[j, pl.ds(chip * 2, 2)].reshape(BLOCK, width)
                a = dot(ctx[pl.ds(starts[t], BLOCK), :], wout[...])
                rbuf[t] = (x.astype(F32) + a + vec(B_OUT)).astype(BF16)

            def norm(t):
                for r0 in range(0, BLOCK, 64):
                    nbuf[t, r0:r0 + 64, :] = layer_norm(rbuf[t, r0:r0 + 64, :].astype(F32), vec(LN2_G), vec(LN2_B)).astype(BF16)

            def up(t):
                for hc in range(hid_chunks):
                    cols_ = slice(hc * width, (hc + 1) * width)
                    hid[t, :, cols_] = gelu(dot(nbuf[t], wup[:, cols_]) + vec(N_FIXED + hc)).astype(BF16)

            def down(t, row_parts):
                for lo, size, parts in row_parts:
                    rows = slice(lo, lo + size)
                    y = jnp.concatenate([dot(hid[t, rows, :], wdown[:, c0:c1]) for c0, c1 in parts], axis=1)
                    y = (rbuf[t, rows, :].astype(F32) + y + vec(B_DOWN)).astype(BF16)
                    for r0 in range(0, size, 64):
                        zbuf[t, lo + r0:lo + r0 + 64, :] = layer_norm(y[r0:r0 + 64].astype(F32), vec(LNF_G), vec(LNF_B)).astype(BF16)

            whole = [(0, width)]
            row_halves = [(0, BLOCK // 2, whole), (BLOCK // 2, BLOCK // 2, whole)]

            resid(0)
            resid(1)
            pool(1, 2 * i + nq - 1)
            norm(0)
            up(0)
            norm(1)
            up(1)
            down(0, [(0, BLOCK, whole)])
            down(1, row_halves)
            pool(0, 2 * i)
            return c

        lax.fori_loop(0, nq // 2, tail, 0)
        return carry

    lax.fori_loop(0, per, one_image, 0)
    finish_pool(per - 1)

    for i in range(6, len(weights)):
        wait_weight(i)
    o = (dot(abuf[...].astype(BF16), pwout[...]) + vec(P_BOUT)).astype(BF16).astype(F32)
    normed = layer_norm(o, vec(P_LN_G), vec(P_LN_B)).astype(BF16)
    emb = o + vec(P_BDOWN)
    for hc in range(hid_chunks):
        cols_ = slice(hc * width, (hc + 1) * width)
        m = gelu(dot(normed, pwup[:, cols_]) + vec(N_FIXED + hid_chunks + hc)).astype(BF16)
        emb = emb + dot(m, pwdown[cols_, :])
    gath[pl.ds(me, 1)] = emb[0:8][None]

    copies = []
    for s in range(1, n):
        copies.append(pltpu.make_async_remote_copy(
            src_ref=gath.at[me],
            dst_ref=gath.at[me],
            send_sem=gsend_sem.at[s],
            recv_sem=grecv_sem.at[me],
            device_id={"cp": (me + s) % n},
            device_id_type=pl.DeviceIdType.MESH,
        ))
    for copy in copies:
        copy.start()
    for j in range(per):
        for copy in sends(j) + forwards(j):
            copy.wait_send()
    for s in range(1, n):
        src = (me + s) % n
        pltpu.make_async_remote_copy(
            src_ref=gath.at[src], dst_ref=gath.at[src], send_sem=gsend_sem.at[s], recv_sem=grecv_sem.at[src],
            device_id={"cp": src}, device_id_type=pl.DeviceIdType.MESH,
        ).wait_recv()
    for copy in copies:
        copy.wait_send()
    for s in range(n):
        out_ref[s * per:(s + 1) * per, :] = gath[s, 0:per, :]


def solution(mesh):
    n = mesh.shape["cp"]

    def device_step(images, ln1_scale, ln1_bias, w_qkv, b_qkv, w_out, b_out, ln2_scale, ln2_bias, w_up, b_up, w_down, b_down, lnf_scale, lnf_bias, pool_probe, pool_wq, pool_bq, pool_wkv, pool_bkv, pool_wout, pool_bout, pool_ln_scale, pool_ln_bias, pool_w_up, pool_b_up, pool_w_down, pool_b_down):
        count, run, width = images.shape
        heads, head_dim = w_qkv.shape[2:]
        mlp = w_up.shape[1]
        per = count // n
        tokens = n * run
        wqkv_t = jnp.transpose(w_qkv, (1, 2, 3, 0)).reshape(3 * width, width)
        wpkv_t = jnp.transpose(pool_wkv, (1, 2, 3, 0)).reshape(2 * width, width)
        wpq_t = jnp.transpose(pool_wq, (1, 2, 0)).reshape(width, width)
        wout2 = w_out.reshape(width, width)
        pwout2 = pool_wout.reshape(width, width)
        smalls = (ln1_scale, ln1_bias, b_out, ln2_scale, ln2_bias, b_down, lnf_scale, lnf_bias, pool_bout, pool_ln_scale, pool_ln_bias, pool_b_down, b_qkv, pool_bq, jnp.transpose(pool_bkv, (1, 0, 2)), b_up, pool_b_up)
        any_spec = pl.BlockSpec(memory_space=pl.ANY)
        vmem_spec = pl.BlockSpec(memory_space=pltpu.VMEM)
        big = (images, wqkv_t, wout2, w_up, w_down, wpkv_t, wpq_t, pwout2, pool_w_up, pool_w_down)
        scratch = [pltpu.VMEM(w.shape, BF16) for w in big[1:]] + [
            pltpu.VMEM((per, n, run, width), BF16),
            pltpu.VMEM((per, heads, LANES, tokens), BF16),
            pltpu.VMEM((per, tokens, width), BF16),
            pltpu.VMEM((per, width, tokens), BF16),
            *[pltpu.VMEM((tokens, BLOCK), F32) for _ in range(4)],
            pltpu.VMEM((2, 2, 8, BLOCK), F32),
            pltpu.VMEM((tokens, width), BF16),
            pltpu.VMEM((2, BLOCK, width), BF16),
            pltpu.VMEM((2, BLOCK, width), BF16),
            pltpu.VMEM((2, BLOCK, width), BF16),
            pltpu.VMEM((2, BLOCK, mlp), BF16),
            pltpu.VMEM((2, BLOCK, width), BF16),
            pltpu.VMEM((16, tokens), F32),
            pltpu.VMEM((tokens, width), BF16),
            pltpu.VMEM((16, width), BF16),
            pltpu.VMEM((2, width, LANES), F32),
            pltpu.VMEM((16, width), F32),
            pltpu.VMEM((n, 8, width), F32),
            pltpu.VMEM((per, 2, run, width), BF16),
            pltpu.VMEM((N_FIXED + 2 * mlp // width, width), F32),
            pltpu.VMEM(pool_probe.shape, BF16),
            *[pltpu.VMEM(v.shape, F32) for v in smalls],
            pltpu.SemaphoreType.DMA((per, n)),
            pltpu.SemaphoreType.DMA((per, n)),
            pltpu.SemaphoreType.DMA((per, 2)),
            pltpu.SemaphoreType.DMA((per, 2)),
            pltpu.SemaphoreType.DMA((len(big) - 1,)),
            pltpu.SemaphoreType.DMA((n,)),
            pltpu.SemaphoreType.DMA((n,)),
            pltpu.SemaphoreType.DMA((N_SMALL + 1,)),
        ]
        return pl.pallas_call(
            functools.partial(kernel, (n, per, heads, head_dim, width, mlp)),
            out_shape=jax.ShapeDtypeStruct((count, width), F32),
            in_specs=[any_spec] * (len(big) + len(smalls) + 1),
            out_specs=vmem_spec,
            scratch_shapes=scratch,
            compiler_params=pltpu.CompilerParams(collective_id=0, has_side_effects=True, vmem_limit_bytes=67043328),
            name="encoder_pool",
        )(*big, *smalls, pool_probe)

    in_specs = (P("dp", "cp", None),) + (P(),) * 27
    return jax.shard_map(device_step, mesh=mesh, in_specs=in_specs, out_specs=P("dp", None), check_vma=False)
```
